32 devices in a mesh: stream: 16 (over z, y, core), tm: 2 (over x).
Axes of the slice: x: 2, y: 2, z: 4, core: 2. Of those that a mesh axis runs over, the one named last changes fastest.
Arguments:
- signal: bfloat16 [32, 2, 1048576], P('stream', None, 'tm'), parts along dimension 0, may hold values from -11 to 11
- taps: float32 [16, 4096], replicated, may hold values from -1.5 to 1.5
Outputs:
- channels_out: float32 [32, 2, 4096, 256], P('stream', None, 'tm'), parts along dimension 0
The draws below stay inside these ranges and needn't reach their ends.
There are 16 independent parts, one for each index of `stream`. The reference program is written for one: setup_inputs(seed, part) draws one part's arguments, and reference() takes and returns one part's arrays. A program takes and returns all parts, laid end to end along the dimension named above; an argument that names none is the same for every part. Nothing has to cross between parts.
All inputs are finite; a program needn't handle non-finite values.
Results may differ from the reference program's by a relative error of at most 0.0003.
Values may be sent and summed in bfloat16 or wider, within the bound.
A program may use at most 128 MiB of HBM per device.

```python
import math
import jax
import jax.numpy as jnp
from jax import lax

CHANNELS = 4096
RADIX = 64
TAPS = 16
STREAMS = 2
FRAMES = 256
SAMPLES = 1048576


def draw_signal(key, part):
    key_noise, key_gain, key_freq, key_level = jax.random.split(key, 4)
    blocks = FRAMES // 8 + 1
    position = jnp.arange(SAMPLES, dtype=jnp.int32)
    which = position // CHANNELS // 8
    noise = jax.random.truncated_normal(key_noise, -4.0, 4.0, (STREAMS, 2, SAMPLES), jnp.float32)
    gains = jnp.exp(jax.random.uniform(key_gain, (STREAMS, blocks), jnp.float32, math.log(0.5), math.log(2.0)))
    envelope = gains[:, which]
    numerators = jax.random.randint(key_freq, (STREAMS, 3), 0, 1 << 20, jnp.int32)
    levels = jax.random.uniform(key_level, (STREAMS, 3), jnp.float32, 0.3, 1.0)
    tone_real = jnp.zeros((STREAMS, SAMPLES), jnp.float32)
    tone_imag = jnp.zeros((STREAMS, SAMPLES), jnp.float32)
    for number in range(3):
        wrapped = jnp.bitwise_and(numerators[:, number][:, None] * position[None, :], (1 << 20) - 1)
        phase = wrapped.astype(jnp.float32) * (2.0 * math.pi / (1 << 20))
        tone_real = tone_real + levels[:, number][:, None] * jnp.cos(phase)
        tone_imag = tone_imag + levels[:, number][:, None] * jnp.sin(phase)
    result = jnp.stack([noise[:, 0] * envelope + tone_real, noise[:, 1] * envelope + tone_imag], axis=1)
    return result.astype(jnp.bfloat16)


def bell_draw(rng, shape, scale, bound, held_as=jnp.bfloat16):
    array = jax.random.normal(rng, shape, jnp.float32) * scale
    return jnp.minimum(jnp.maximum(array, -bound), bound).astype(held_as)


def setup_inputs(seed: int = 0, part: int = 0) -> dict:
    key_of = jax.random.split(jax.random.key(seed), 3)
    part_keys = jax.random.split(jax.random.fold_in(key_of[2], part), 3)
    signal = draw_signal(jax.random.fold_in(jax.random.fold_in(key_of[2], part), 71), part)
    taps = bell_draw(key_of[1], (TAPS, CHANNELS), TAPS ** -0.5, 1.5, jnp.float32)
    return {"signal": signal, "taps": taps}


def reference(signal, taps):
    streams = signal.shape[0]
    frames = signal.astype(jnp.float32).reshape(streams, 2, FRAMES, CHANNELS)
    padded = jnp.pad(frames, ((0, 0), (0, 0), (TAPS - 1, 0), (0, 0)))
    filtered = jnp.zeros((streams, 2, FRAMES, CHANNELS), jnp.float32)
    for tap_index in range(TAPS):
        start = TAPS - 1 - tap_index
        filtered = filtered + taps[tap_index] * padded[:, :, start:start + FRAMES, :]
    spectrum = jnp.fft.fft(lax.complex(filtered[:, 0], filtered[:, 1]), axis=-1) / RADIX
    real_part = jnp.real(spectrum)
    imag_part = jnp.imag(spectrum)
    power = lax.optimization_barrier(jnp.mean(real_part * real_part + imag_part * imag_part, axis=1))
    factor = 1.0 / jnp.sqrt(power + 1.0)
    stacked = jnp.stack([real_part * factor[:, None, :], imag_part * factor[:, None, :]], axis=1)
    return jnp.transpose(stacked, (0, 1, 3, 2))
```

```python
import functools
import math

import jax
import jax.numpy as jnp
import numpy as np
from jax import lax
from jax.experimental import pallas as pl
from jax.experimental.pallas import tpu as pltpu
from jax.sharding import PartitionSpec as P

LANES = 128
GROUP = 4
BATCH = 2 * GROUP
PAIR = 2
POWER = 6
SCALE = 64.0


def angles(height, breadth, modulus):
    product = np.arange(height)[:, None] * np.arange(breadth)[None, :] % modulus
    return product * (2.0 * math.pi / modulus)


def split(table):
    high = table.astype(np.float32).astype(jnp.bfloat16)
    low = (table - high.astype(np.float64)).astype(np.float32).astype(jnp.bfloat16)
    return high, low


def first_table(rows):
    turn = angles(rows, rows, rows)
    cos, sin = np.cos(turn), np.sin(turn)
    whole = np.block([[cos, sin], [-sin, cos]])
    woven = whole.reshape(2 * rows, 2, rows).transpose(0, 2, 1).reshape(2 * rows, 2 * rows)
    high, low = split(np.kron(np.eye(GROUP), woven))
    return np.concatenate([high, low, high], axis=1)


def second_table(channels, parts):
    turn = angles(LANES, LANES, LANES)
    scale = 1.0 / math.isqrt(channels)
    cos, sin = np.cos(turn) * scale, np.sin(turn) * scale
    each = LANES // parts
    blocks = []
    for part in range(parts):
        pick = slice(part * each, (part + 1) * each)
        blocks.append(np.block([[cos[pick], sin[pick]], [-sin[pick], cos[pick]]]))
    high, low = split(np.concatenate(blocks, axis=0))
    table = np.concatenate([high, low, high], axis=1)
    return np.concatenate([table, table], axis=0)


def encode(value):
    value = value * SCALE
    square = value * jnp.abs(value)
    return (square * (square * square)).astype(jnp.bfloat16)


def decode(code):
    value = code.astype(jnp.float32)
    size = jnp.exp(jnp.log(jnp.abs(value)) * (1.0 / POWER)) * (1.0 / SCALE)
    return jnp.where(value < 0.0, -size, size)


def halves(value):
    high = value.astype(jnp.bfloat16)
    low = (value - high.astype(jnp.float32)).astype(jnp.bfloat16)
    return high, low


def channelize(parts, streams, frames, rows, depth, x_hbm, taps_ref, first_ref, cos_ref, sin_ref,
               second_ref, out_ref, xbuf, halo, wide, grid, zr, zi, own, send, recv,
               x_sem, halo_send, halo_recv, send_sem, recv_sem):
    me = lax.axis_index("tm")
    each = LANES // parts
    past = depth - 1
    pitch = zr.shape[0] // rows
    steps = rows // PAIR

    barrier = pltpu.get_barrier_semaphore()
    for k in range(1, parts):
        pl.semaphore_signal(barrier, inc=1, device_id={"tm": lax.rem(me + k, parts)},
                            device_id_type=pl.DeviceIdType.MESH)
    load = pltpu.make_async_copy(x_hbm.at[0], xbuf, x_sem)
    load.start()
    pl.semaphore_wait(barrier, parts - 1)

    def edge(s):
        return pltpu.make_async_remote_copy(
            src_ref=x_hbm.at[s, pl.ds(frames - past, past)], dst_ref=halo.at[s],
            send_sem=halo_send.at[s], recv_sem=halo_recv.at[s],
            device_id={"tm": lax.rem(me + 1, parts)}, device_id_type=pl.DeviceIdType.MESH)

    def piece(s, k, step):
        return pltpu.make_async_remote_copy(
            src_ref=send.at[s, k - 1, step], dst_ref=recv.at[s, k - 1, step],
            send_sem=send_sem.at[s, k - 1, step], recv_sem=recv_sem.at[s, k - 1, step],
            device_id={"tm": lax.rem(me + k, parts)}, device_id_type=pl.DeviceIdType.MESH)

    @pl.when(me < parts - 1)
    def _():
        for s in range(streams):
            edge(s).start()

    def first_stage(step):
        base = pl.multiple_of(step * BATCH, BATCH)
        for block in range(2 * rows // 8):
            sub = slice(block * 8, block * 8 + 8)
            data = [wide[base + i, sub, :] for i in range(BATCH + past)]
            taps = [taps_ref[k, sub, :] for k in range(depth)]
            for t in range(BATCH):
                total = taps[0] * data[t + past]
                for k in range(1, depth):
                    total = total + taps[k] * data[t + past - k]
                row = (t % GROUP) * 2 * rows + block * 8
                lane = (t // GROUP) * LANES
                grid[row : row + 8, lane : lane + LANES] = total
        high, low = halves(grid[...])
        out = jnp.dot(first_ref[...], jnp.concatenate([high, high, low], axis=0),
                      preferred_element_type=jnp.float32)
        cos, sin = cos_ref[...], sin_ref[...]
        for t in range(BATCH):
            row = (t % GROUP) * 2 * rows
            lane = (t // GROUP) * LANES
            real = out[row : row + rows, lane : lane + LANES]
            imag = out[row + rows : row + 2 * rows, lane : lane + LANES]
            pick = pl.ds(base + t, rows, stride=pitch)
            zr[pick, :] = real * cos + imag * sin
            zi[pick, :] = imag * cos - real * sin

    def second_stage(s, step):
        pieces = []
        for i in range(PAIR):
            pick = pl.ds(pl.multiple_of((step * PAIR + i) * pitch, 8), frames)
            pieces.append(jnp.concatenate([zr[pick, :], zi[pick, :]], axis=1))
        high, low = halves(jnp.concatenate(pieces, axis=0))
        top = pl.ds(pl.multiple_of(me * 2 * each, 2 * each), 2 * LANES)
        out = lax.dot_general(second_ref[top, :], jnp.concatenate([high, high, low], axis=1),
                              (((1,), (1,)), ((), ())), preferred_element_type=jnp.float32)
        for i in range(PAIR):
            lane = slice(i * frames, (i + 1) * frames)
            for p in range(2):
                own[s, p, step * PAIR + i] = out[p * each : (p + 1) * each, lane]
                for k in range(1, parts):
                    row = (2 * k + p) * each
                    send[s, k - 1, step, p, i] = encode(out[row : row + each, lane])

    def finish(s, step):
        for k in range(1, parts):
            piece(s, k, step).wait_recv()
        for i in range(PAIR):
            c = step * PAIR + i
            data = [[own[s, p, c] for p in range(2)]]
            for k in range(1, parts):
                data.append([decode(recv[s, k - 1, step, p, i]) for p in range(2)])
            square = sum(d[0] * d[0] + d[1] * d[1] for d in data)
            power = jnp.sum(square, axis=1, keepdims=True)
            factor = lax.rsqrt(power * (1.0 / (frames * parts)) + 1.0)
            for k in range(parts):
                source = lax.rem(me + parts - k, parts) * (frames // LANES)
                for p in range(2):
                    result = data[k][p] * factor
                    for j in range(frames // LANES):
                        lane = slice(j * LANES, (j + 1) * LANES)
                        out_ref[s, p, source + j, pl.ds(c, each, stride=rows), :] = result[:, lane]

    for s in range(streams):
        load.wait()

        @pl.loop(0, frames // BATCH)
        def _(step):
            base = pl.multiple_of(step * BATCH, BATCH)
            wide[pl.ds(base + past, BATCH)] = xbuf[pl.ds(base, BATCH)].astype(jnp.float32)

        if s + 1 < streams:
            load = pltpu.make_async_copy(x_hbm.at[s + 1], xbuf, x_sem)
            load.start()

        front = -(-past // BATCH)

        @pl.loop(front, frames // BATCH)
        def _(step):
            first_stage(step)

        @pl.when(me > 0)
        def _():
            edge(s).wait_recv()
            wide[:past] = halo[s].astype(jnp.float32)

        @pl.when(me == 0)
        def _():
            wide[:past] = jnp.zeros((past, 2 * rows, LANES), jnp.float32)

        @pl.loop(0, front)
        def _(step):
            first_stage(step)

        @pl.loop(0, steps)
        def _(step):
            second_stage(s, step)

            @pl.when(step > 0)
            def _():
                for k in range(1, parts):
                    piece(s, k, step - 1).start()

        for k in range(1, parts):
            piece(s, k, steps - 1).start()

    for s in range(streams):

        @pl.loop(0, steps)
        def _(step):
            finish(s, step)

    for s in range(streams):

        @pl.loop(0, steps)
        def _(step):
            for k in range(1, parts):
                piece(s, k, step).wait_send()

    @pl.when(me < parts - 1)
    def _():
        for s in range(streams):
            edge(s).wait_send()


def deliver(streams, spans, planes_ref, out_ref, sem):
    copies = []
    for s in range(streams):
        for p in range(2):
            for j in range(spans):
                lane = slice(j * LANES, (j + 1) * LANES)
                copies.append(pltpu.make_async_copy(
                    planes_ref.at[s, p, j], out_ref.at[s, p, :, lane], sem.at[s, p, j]))
    for copy in copies:
        copy.start()
    for copy in copies:
        copy.wait()


def shards(parts, signal, taps):
    streams = signal.shape[0]
    depth, channels = taps.shape
    rows = channels // LANES
    frames = signal.shape[2] // channels
    each = LANES // parts
    chunks = signal.shape[2] // LANES
    x = signal.reshape(streams, 2, chunks, LANES).transpose(0, 2, 1, 3)
    x = x.reshape(streams, frames, 2 * rows, LANES)
    taps = jnp.repeat(taps.reshape(depth, rows, LANES), 2, axis=1)
    twist = angles(rows, LANES, channels)
    cos, sin = jnp.asarray(np.cos(twist), jnp.float32), jnp.asarray(np.sin(twist), jnp.float32)
    first = jnp.asarray(first_table(rows))
    second = jnp.asarray(second_table(channels, parts))
    steps = rows // PAIR
    pitch = frames + 8
    vmem = pl.BlockSpec(memory_space=pltpu.VMEM)
    code = (streams, parts - 1, steps, 2, PAIR, each, frames)
    spans = frames * parts // LANES
    width = 2 * rows * LANES * frames
    limit = (8 << 20) + 2 * width + 4 * width + 4 * width * 9 // 8 + 8 * width * streams * (parts + 1) // parts
    planes = pl.pallas_call(
        functools.partial(channelize, parts, streams, frames, rows, depth),
        in_specs=[pl.BlockSpec(memory_space=pl.ANY)] + [vmem] * 5,
        out_specs=vmem,
        out_shape=jax.ShapeDtypeStruct((streams, 2, spans, channels // parts, LANES), jnp.float32),
        scratch_shapes=[
            pltpu.VMEM((frames, 2 * rows, LANES), jnp.bfloat16),
            pltpu.VMEM((streams, depth - 1, 2 * rows, LANES), jnp.bfloat16),
            pltpu.VMEM((depth - 1 + frames, 2 * rows, LANES), jnp.float32),
            pltpu.VMEM((2 * GROUP * rows, 2 * LANES), jnp.float32),
            pltpu.VMEM((rows * pitch, LANES), jnp.float32),
            pltpu.VMEM((rows * pitch, LANES), jnp.float32),
            pltpu.VMEM((streams, 2, rows, each, frames), jnp.float32),
            pltpu.VMEM(code, jnp.bfloat16),
            pltpu.VMEM(code, jnp.bfloat16),
            pltpu.SemaphoreType.DMA,
            pltpu.SemaphoreType.DMA((streams,)),
            pltpu.SemaphoreType.DMA((streams,)),
            pltpu.SemaphoreType.DMA((streams, parts - 1, steps)),
            pltpu.SemaphoreType.DMA((streams, parts - 1, steps)),
        ],
        compiler_params=pltpu.CompilerParams(
            vmem_limit_bytes=limit, collective_id=0, has_side_effects=True),
        cost_estimate=pl.CostEstimate(flops=16 * 10**9, bytes_accessed=16 << 20, transcendentals=0),
        name="channelize",
    )(x, taps, first, cos, sin, second)
    return pl.pallas_call(
        functools.partial(deliver, streams, spans),
        in_specs=[vmem],
        out_specs=pl.BlockSpec(memory_space=pl.ANY),
        out_shape=jax.ShapeDtypeStruct((streams, 2, channels // parts, spans * LANES), jnp.float32),
        scratch_shapes=[pltpu.SemaphoreType.DMA((streams, 2, spans))],
        compiler_params=pltpu.CompilerParams(vmem_limit_bytes=20 << 20),
        cost_estimate=pl.CostEstimate(flops=10**6, bytes_accessed=16 << 20, transcendentals=0),
        name="deliver",
    )(planes)


def solution(mesh):
    in_specs = (P("stream", None, "tm"), P())
    out_specs = P("stream", None, "tm", None)
    body = functools.partial(shards, mesh.shape["tm"])
    return jax.shard_map(body, mesh=mesh, in_specs=in_specs, out_specs=out_specs, check_vma=False)
```

```python
import functools
import math

import jax
import jax.numpy as jnp
import numpy as np
from jax import lax
from jax.experimental import pallas as pl
from jax.experimental.pallas import tpu as pltpu
from jax.sharding import PartitionSpec as P

LANES = 128
GROUP = 4
BATCH = 2 * GROUP
PAIR = 2
POWER = 6
SCALE = 64.0


def angles(height, breadth, modulus):
    product = np.arange(height)[:, None] * np.arange(breadth)[None, :] % modulus
    return product * (2.0 * math.pi / modulus)


def split(table):
    high = table.astype(np.float32).astype(jnp.bfloat16)
    low = (table - high.astype(np.float64)).astype(np.float32).astype(jnp.bfloat16)
    return high, low


def first_table(rows):
    turn = angles(rows, rows, rows)
    cos, sin = np.cos(turn), np.sin(turn)
    whole = np.block([[cos, sin], [-sin, cos]])
    woven = whole.reshape(2 * rows, 2, rows).transpose(0, 2, 1).reshape(2 * rows, 2 * rows)
    high, low = split(np.kron(np.eye(GROUP), woven))
    return np.concatenate([high, low, high], axis=1)


def second_table(channels, parts):
    turn = angles(LANES, LANES, LANES)
    scale = 1.0 / math.isqrt(channels)
    cos, sin = np.cos(turn) * scale, np.sin(turn) * scale
    each = LANES // parts
    blocks = []
    for part in range(parts):
        pick = slice(part * each, (part + 1) * each)
        blocks.append(np.block([[cos[pick], sin[pick]], [-sin[pick], cos[pick]]]))
    high, low = split(np.concatenate(blocks, axis=0))
    table = np.concatenate([high, low, high], axis=1)
    return np.concatenate([table, table], axis=0)


def encode(value):
    value = value * SCALE
    square = value * jnp.abs(value)
    return (square * (square * square)).astype(jnp.bfloat16)


def decode(code):
    value = code.astype(jnp.float32)
    size = jnp.exp(jnp.log(jnp.abs(value)) * (1.0 / POWER)) * (1.0 / SCALE)
    return jnp.where(value < 0.0, -size, size)


def halves(value):
    high = value.astype(jnp.bfloat16)
    low = (value - high.astype(jnp.float32)).astype(jnp.bfloat16)
    return high, low


def channelize(parts, streams, frames, rows, depth, x_hbm, taps_hbm, first_hbm, cos_hbm, sin_hbm,
               second_hbm, out_ref, xbuf, taps_raw, taps_ref, first_ref, cos_ref, sin_ref, second_ref,
               halo, wide, grid, zr, zi, own, send, recv,
               x_sem, table_sem, halo_send, halo_recv, send_sem, recv_sem):
    me = lax.axis_index("tm")
    each = LANES // parts
    past = depth - 1
    pitch = zr.shape[0] // rows
    steps = rows // PAIR
    spans = frames * parts // LANES
    reach = taps_ref.shape[0] // depth

    barrier = pltpu.get_barrier_semaphore()
    for k in range(1, parts):
        pl.semaphore_signal(barrier, inc=1, device_id={"tm": lax.rem(me + k, parts)},
                            device_id_type=pl.DeviceIdType.MESH)
    load = pltpu.make_async_copy(x_hbm.at[0], xbuf, x_sem)
    load.start()
    tables = [
        pltpu.make_async_copy(source, target, table_sem.at[i])
        for i, (source, target) in enumerate([
            (taps_hbm, taps_raw), (first_hbm, first_ref), (cos_hbm, cos_ref),
            (sin_hbm, sin_ref), (second_hbm, second_ref)])
    ]
    for table in tables:
        table.start()
    pl.semaphore_wait(barrier, parts - 1)

    def edge(s):
        return pltpu.make_async_remote_copy(
            src_ref=x_hbm.at[s, pl.ds(frames - past, past)], dst_ref=halo.at[s],
            send_sem=halo_send.at[s], recv_sem=halo_recv.at[s],
            device_id={"tm": lax.rem(me + 1, parts)}, device_id_type=pl.DeviceIdType.MESH)

    def piece(s, k, step):
        return pltpu.make_async_remote_copy(
            src_ref=send.at[s, k - 1, step], dst_ref=recv.at[s, k - 1, step],
            send_sem=send_sem.at[s, k - 1, step], recv_sem=recv_sem.at[s, k - 1, step],
            device_id={"tm": lax.rem(me + k, parts)}, device_id_type=pl.DeviceIdType.MESH)

    @pl.when(me < parts - 1)
    def _():
        for s in range(streams):
            edge(s).start()

    for table in tables:
        table.wait()

    @pl.loop(0, rows)
    def _(n):
        for g in range(depth // 8):
            for p in range(2):
                row = pl.ds(g * 8 * reach + 2 * n + p, 8, stride=reach)
                taps_ref[row, :] = taps_raw[g, n]

    def first_stage(step):
        base = pl.multiple_of(step * BATCH, BATCH)
        for block in range(2 * rows // 8):
            sub = slice(block * 8, block * 8 + 8)
            data = [wide[base + i, sub, :] for i in range(BATCH + past)]
            taps = [taps_ref[k * reach + block * 8 : k * reach + block * 8 + 8, :] for k in range(depth)]
            for t in range(BATCH):
                total = taps[0] * data[t + past]
                for k in range(1, depth):
                    total = total + taps[k] * data[t + past - k]
                row = (t % GROUP) * 2 * rows + block * 8
                lane = (t // GROUP) * LANES
                grid[row : row + 8, lane : lane + LANES] = total
        high, low = halves(grid[...])
        out = jnp.dot(first_ref[...], jnp.concatenate([high, high, low], axis=0),
                      preferred_element_type=jnp.float32)
        cos, sin = cos_ref[...], sin_ref[...]
        for t in range(BATCH):
            row = (t % GROUP) * 2 * rows
            lane = (t // GROUP) * LANES
            real = out[row : row + rows, lane : lane + LANES]
            imag = out[row + rows : row + 2 * rows, lane : lane + LANES]
            pick = pl.ds(base + t, rows, stride=pitch)
            zr[pick, :] = real * cos + imag * sin
            zi[pick, :] = imag * cos - real * sin

    def second_stage(s, step):
        pieces = []
        for i in range(PAIR):
            pick = pl.ds(pl.multiple_of((step * PAIR + i) * pitch, 8), frames)
            pieces.append(jnp.concatenate([zr[pick, :], zi[pick, :]], axis=1))
        high, low = halves(jnp.concatenate(pieces, axis=0))
        top = pl.ds(pl.multiple_of(me * 2 * each, 2 * each), 2 * LANES)
        out = lax.dot_general(second_ref[top, :], jnp.concatenate([high, high, low], axis=1),
                              (((1,), (1,)), ((), ())), preferred_element_type=jnp.float32)
        for i in range(PAIR):
            lane = slice(i * frames, (i + 1) * frames)
            for p in range(2):
                own[s, p, step * PAIR + i] = out[p * each : (p + 1) * each, lane]
                for k in range(1, parts):
                    row = (2 * k + p) * each
                    send[s, k - 1, step, p, i] = encode(out[row : row + each, lane])

    def finish(s, step):
        for k in range(1, parts):
            piece(s, k, step).wait_recv()
        for i in range(PAIR):
            c = step * PAIR + i
            data = [[own[s, p, c] for p in range(2)]]
            for k in range(1, parts):
                data.append([decode(recv[s, k - 1, step, p, i]) for p in range(2)])
            square = sum(d[0] * d[0] + d[1] * d[1] for d in data)
            power = jnp.sum(square, axis=1, keepdims=True)
            factor = lax.rsqrt(power * (1.0 / (frames * parts)) + 1.0)
            for k in range(parts):
                source = lax.rem(me + parts - k, parts) * (frames // LANES)
                top = (c // 8) * (8 * spans) + c % 8
                for p in range(2):
                    result = data[k][p] * factor
                    for j in range(frames // LANES):
                        lane = slice(j * LANES, (j + 1) * LANES)
                        row = pl.ds(top + (source + j) * 8, each, stride=rows * spans)
                        out_ref[s, p, row, :] = result[:, lane]

    for s in range(streams):
        load.wait()

        @pl.loop(0, frames // BATCH)
        def _(step):
            base = pl.multiple_of(step * BATCH, BATCH)
            wide[pl.ds(base + past, BATCH)] = xbuf[pl.ds(base, BATCH)].astype(jnp.float32)

        if s + 1 < streams:
            load = pltpu.make_async_copy(x_hbm.at[s + 1], xbuf, x_sem)
            load.start()

        front = -(-past // BATCH)

        @pl.loop(front, frames // BATCH)
        def _(step):
            first_stage(step)

        @pl.when(me > 0)
        def _():
            edge(s).wait_recv()
            wide[:past] = halo[s].astype(jnp.float32)

        @pl.when(me == 0)
        def _():
            wide[:past] = jnp.zeros((past, 2 * rows, LANES), jnp.float32)

        @pl.loop(0, front)
        def _(step):
            first_stage(step)

        @pl.loop(0, steps)
        def _(step):
            second_stage(s, step)

            @pl.when(step > 0)
            def _():
                for k in range(1, parts):
                    piece(s, k, step - 1).start()

        for k in range(1, parts):
            piece(s, k, steps - 1).start()

    for s in range(streams):

        @pl.loop(0, steps)
        def _(step):
            finish(s, step)

    for s in range(streams):

        @pl.loop(0, steps)
        def _(step):
            for k in range(1, parts):
                piece(s, k, step).wait_send()

    @pl.when(me < parts - 1)
    def _():
        for s in range(streams):
            edge(s).wait_send()


def shards(parts, signal, taps):
    streams = signal.shape[0]
    depth, channels = taps.shape
    rows = channels // LANES
    frames = signal.shape[2] // channels
    each = LANES // parts
    chunks = signal.shape[2] // LANES
    x = signal.reshape(streams, 2, chunks, LANES).transpose(0, 2, 1, 3)
    x = x.reshape(streams, frames, 2 * rows, LANES)
    taps = taps.reshape(depth // 8, 8, rows, LANES).transpose(0, 2, 1, 3)
    twist = angles(rows, LANES, channels)
    cos, sin = jnp.asarray(np.cos(twist), jnp.float32), jnp.asarray(np.sin(twist), jnp.float32)
    first = jnp.asarray(first_table(rows))
    second = jnp.asarray(second_table(channels, parts))
    steps = rows // PAIR
    pitch = frames + 8
    reach = 2 * rows + 8
    spans = frames * parts // LANES
    tiles = channels // parts // 8
    width = 2 * rows * LANES * frames
    limit = (8 << 20) + 2 * width + 4 * width + 4 * width * 9 // 8 + 8 * width * streams * (parts + 1) // parts
    hbm = pl.BlockSpec(memory_space=pltpu.HBM)
    code = (streams, parts - 1, steps, 2, PAIR, each, frames)
    operands = [x, taps, first, cos, sin, second]
    operands = [pltpu.with_memory_space_constraint(a, pltpu.HBM) for a in operands]
    out = pl.pallas_call(
        functools.partial(channelize, parts, streams, frames, rows, depth),
        in_specs=[hbm] * 6,
        out_specs=pl.BlockSpec(memory_space=pltpu.VMEM),
        out_shape=pltpu.VMEM((streams, 2, 8 * tiles * spans, LANES), jnp.float32),
        scratch_shapes=[
            pltpu.VMEM((frames, 2 * rows, LANES), jnp.bfloat16),
            pltpu.VMEM(taps.shape, jnp.float32),
            pltpu.VMEM((depth * reach, LANES), jnp.float32),
            pltpu.VMEM(first.shape, jnp.bfloat16),
            pltpu.VMEM(cos.shape, jnp.float32),
            pltpu.VMEM(sin.shape, jnp.float32),
            pltpu.VMEM(second.shape, jnp.bfloat16),
            pltpu.VMEM((streams, depth - 1, 2 * rows, LANES), jnp.bfloat16),
            pltpu.VMEM((depth - 1 + frames, 2 * rows, LANES), jnp.float32),
            pltpu.VMEM((2 * GROUP * rows, 2 * LANES), jnp.float32),
            pltpu.VMEM((rows * pitch, LANES), jnp.float32),
            pltpu.VMEM((rows * pitch, LANES), jnp.float32),
            pltpu.VMEM((streams, 2, rows, each, frames), jnp.float32),
            pltpu.VMEM(code, jnp.bfloat16),
            pltpu.VMEM(code, jnp.bfloat16),
            pltpu.SemaphoreType.DMA,
            pltpu.SemaphoreType.DMA((5,)),
            pltpu.SemaphoreType.DMA((streams,)),
            pltpu.SemaphoreType.DMA((streams,)),
            pltpu.SemaphoreType.DMA((streams, parts - 1, steps)),
            pltpu.SemaphoreType.DMA((streams, parts - 1, steps)),
        ],
        compiler_params=pltpu.CompilerParams(
            vmem_limit_bytes=limit, collective_id=0, has_side_effects=True),
        cost_estimate=pl.CostEstimate(flops=16 * 10**9, bytes_accessed=16 << 20, transcendentals=0),
        name="channelize",
    )(*operands)
    out = out.reshape(streams, 2, tiles, spans, 8, LANES).transpose(0, 1, 2, 4, 3, 5)
    return out.reshape(streams, 2, 8 * tiles, spans * LANES)


def solution(mesh):
    in_specs = (P("stream", None, "tm"), P())
    out_specs = P("stream", None, "tm", None)
    body = functools.partial(shards, mesh.shape["tm"])
    return jax.shard_map(body, mesh=mesh, in_specs=in_specs, out_specs=out_specs, check_vma=False)
```

```python
import functools
import math

import jax
import jax.numpy as jnp
import numpy as np
from jax import lax
from jax.experimental import pallas as pl
from jax.experimental.pallas import tpu as pltpu
from jax.sharding import PartitionSpec as P

LANES = 128
GROUP = 4
BATCH = 2 * GROUP
SPAN = 64
WIDE = 2 * LANES
POWER = 6
SCALE = 64.0


def angles(height, breadth, modulus):
    product = np.arange(height)[:, None] * np.arange(breadth)[None, :] % modulus
    return product * (2.0 * math.pi / modulus)


def split(table):
    high = table.astype(np.float32).astype(jnp.bfloat16)
    low = (table - high.astype(np.float64)).astype(np.float32).astype(jnp.bfloat16)
    return high, low


def first_table(rows):
    turn = angles(rows, rows, rows)
    cos, sin = np.cos(turn), np.sin(turn)
    whole = np.block([[cos, sin], [-sin, cos]])
    woven = whole.reshape(2 * rows, 2, rows).transpose(0, 2, 1).reshape(2 * rows, 2 * rows)
    high, low = split(np.kron(np.eye(GROUP), woven))
    return np.concatenate([high, low, high], axis=1)


def second_table(channels, parts):
    turn = angles(LANES, LANES, LANES)
    scale = 1.0 / math.isqrt(channels)
    cos, sin = np.cos(turn) * scale, np.sin(turn) * scale
    each = LANES // parts
    blocks = []
    for part in range(parts):
        pick = slice(part * each, (part + 1) * each)
        blocks.append(np.block([[cos[pick], sin[pick]], [-sin[pick], cos[pick]]]))
    high, low = split(np.concatenate(blocks, axis=0))
    table = np.concatenate([high, low, high], axis=1)
    return np.concatenate([table, table], axis=0)


def encode(value):
    value = value * SCALE
    square = value * jnp.abs(value)
    return (square * (square * square)).astype(jnp.bfloat16)


def decode(code):
    value = code.astype(jnp.float32)
    size = jnp.exp(jnp.log(jnp.abs(value)) * (1.0 / POWER)) * (1.0 / SCALE)
    return jnp.where(value < 0.0, -size, size)


def halves(value):
    high = value.astype(jnp.bfloat16)
    low = (value - high.astype(jnp.float32)).astype(jnp.bfloat16)
    return high, low


def channelize(parts, streams, frames, rows, depth, x_hbm, taps_hbm, first_hbm, cos_hbm, sin_hbm,
               second_hbm, out_ref, xbuf, taps_raw, taps_ref, first_ref, cos_ref, sin_ref, second_ref,
               halo, wide, grid, zr, zi, own, send, recv, own_over, send_over, recv_over,
               x_sem, table_sem, halo_send, halo_recv, send_sem, recv_sem, over_send, over_recv):
    me = lax.axis_index("tm")
    each = LANES // parts
    past = depth - 1
    over = -(-past // BATCH) * BATCH
    blocks = frames // SPAN
    quad = WIDE // SPAN
    steps = rows // quad
    group = WIDE // over
    spans = frames * parts // LANES
    reach = taps_ref.shape[0] // depth
    bounds = [max(b * SPAN - over, 0) for b in range(blocks)] + [frames]

    barrier = pltpu.get_barrier_semaphore()
    for k in range(1, parts):
        pl.semaphore_signal(barrier, inc=1, device_id={"tm": lax.rem(me + k, parts)},
                            device_id_type=pl.DeviceIdType.MESH)

    def load(s, b):
        pick = pl.ds(bounds[b], bounds[b + 1] - bounds[b])
        return pltpu.make_async_copy(x_hbm.at[s, pick], xbuf.at[pick], x_sem.at[b])

    def edge():
        return pltpu.make_async_remote_copy(
            src_ref=x_hbm.at[0, pl.ds(frames - past, past)], dst_ref=halo,
            send_sem=halo_send, recv_sem=halo_recv,
            device_id={"tm": lax.rem(me + 1, parts)}, device_id_type=pl.DeviceIdType.MESH)

    def piece(s, k, b, step):
        return pltpu.make_async_remote_copy(
            src_ref=send.at[s, k - 1, b, step], dst_ref=recv.at[s, k - 1, b, step],
            send_sem=send_sem.at[s, k - 1, b, step], recv_sem=recv_sem.at[s, k - 1, b, step],
            device_id={"tm": lax.rem(me + k, parts)}, device_id_type=pl.DeviceIdType.MESH)

    def overhang(s, k):
        return pltpu.make_async_remote_copy(
            src_ref=send_over.at[s - 1, k - 1], dst_ref=recv_over.at[s - 1, k - 1],
            send_sem=over_send.at[s - 1, k - 1], recv_sem=over_recv.at[s - 1, k - 1],
            device_id={"tm": lax.rem(me + k, parts)}, device_id_type=pl.DeviceIdType.MESH)

    load(0, blocks - 1).start()
    tables = [
        pltpu.make_async_copy(source, target, table_sem.at[i])
        for i, (source, target) in enumerate([
            (taps_hbm, taps_raw), (first_hbm, first_ref), (cos_hbm, cos_ref),
            (sin_hbm, sin_ref), (second_hbm, second_ref)])
    ]
    for table in tables:
        table.start()
    for b in reversed(range(blocks - 1)):
        load(0, b).start()
    pl.semaphore_wait(barrier, parts - 1)

    @pl.when(me < parts - 1)
    def _():
        edge().start()

    for table in tables:
        table.wait()

    @pl.loop(0, rows)
    def _(n):
        for g in range(depth // 8):
            for p in range(2):
                row = pl.ds(g * 8 * reach + 2 * n + p, 8, stride=reach)
                taps_ref[row, :] = taps_raw[g, n]

    wide[past + frames :] = jnp.zeros((over, 2 * rows, LANES), jnp.float32)

    def widen(s, b):
        load(s, b).wait()

        @pl.loop(bounds[b] // BATCH, bounds[b + 1] // BATCH)
        def _(step):
            base = pl.multiple_of(step * BATCH, BATCH)
            wide[pl.ds(base + past, BATCH)] = xbuf[pl.ds(base, BATCH)].astype(jnp.float32)

    def first_stage(frame, slot, pitch):
        for block in range(2 * rows // 8):
            sub = slice(block * 8, block * 8 + 8)
            data = [wide[frame + i, sub, :] for i in range(BATCH + past)]
            taps = [taps_ref[k * reach + block * 8 : k * reach + block * 8 + 8, :]
                    for k in range(depth)]
            for t in range(BATCH):
                total = taps[0] * data[t + past]
                for k in range(1, depth):
                    total = total + taps[k] * data[t + past - k]
                row = (t % GROUP) * 2 * rows + block * 8
                lane = (t // GROUP) * LANES
                grid[row : row + 8, lane : lane + LANES] = total
        high, low = halves(grid[...])
        out = jnp.dot(first_ref[...], jnp.concatenate([high, high, low], axis=0),
                      preferred_element_type=jnp.float32)
        cos, sin = cos_ref[...], sin_ref[...]
        for t in range(BATCH):
            row = (t % GROUP) * 2 * rows
            lane = (t // GROUP) * LANES
            real = out[row : row + rows, lane : lane + LANES]
            imag = out[row + rows : row + 2 * rows, lane : lane + LANES]
            pick = pl.ds(slot + t, rows, stride=pitch)
            zr[pick, :] = real * cos + imag * sin
            zi[pick, :] = imag * cos - real * sin

    def second_stage(step, count, length, pitch):
        pieces = []
        for i in range(count):
            pick = pl.ds(pl.multiple_of((step * count + i) * pitch, 8), length)
            pieces.append(jnp.concatenate([zr[pick, :], zi[pick, :]], axis=1))
        high, low = halves(jnp.concatenate(pieces, axis=0))
        top = pl.ds(pl.multiple_of(me * 2 * each, 2 * each), 2 * LANES)
        return lax.dot_general(second_ref[top, :], jnp.concatenate([high, high, low], axis=1),
                               (((1,), (1,)), ((), ())), preferred_element_type=jnp.float32)

    def keep(out, mine, theirs):
        for j in range(WIDE // LANES):
            lane = slice(j * LANES, (j + 1) * LANES)
            for p in range(2):
                mine[j, p] = out[p * each : (p + 1) * each, lane]
                for k in range(1, parts):
                    row = (2 * k + p) * each
                    theirs[k - 1][j, p] = encode(out[row : row + each, lane])

    def finish(s, step):
        lanes = lax.broadcasted_iota(jnp.int32, (each, LANES), 1)
        for k in range(1, parts):
            for b in range(blocks):
                piece(s, k, b, step).wait_recv()

        def fetch(k, b, j, p):
            if k == 0:
                return own[s, b, step, j, p]
            return decode(recv[s, k - 1, b, step, j, p])

        def hung(k, c, p):
            at, slot = c // group, (c % group) // (LANES // over)
            if k == 0:
                value = own_over[s - 1, at, slot, p]
            else:
                value = decode(recv_over[s - 1, k - 1, at, slot, p])
            turn = lax.rem(LANES - (c % (LANES // over)) * over, LANES)
            return jnp.where(lanes < over, pltpu.roll(value, turn, 1), 0.0)

        for j in range(WIDE // LANES):
            whole = [[[], []] for _ in range(LANES // SPAN)]
            for k in range(parts):
                for p in range(2):
                    for u in range(frames // LANES):
                        low, high = fetch(k, 2 * u, j, p), fetch(k, 2 * u + 1, j, p)
                        left = lanes < SPAN
                        whole[0][p].append(jnp.where(left, low, pltpu.roll(high, SPAN, 1)))
                        whole[1][p].append(jnp.where(left, pltpu.roll(low, SPAN, 1), high))
            for i in range(LANES // SPAN):
                c = step * quad + j * (LANES // SPAN) + i
                data = whole[i]
                if s > 0:
                    for k in range(parts):
                        source = lax.rem(me + parts - k, parts)
                        for p in range(2):
                            extra = jnp.where(source > 0, hung((k + 1) % parts, c, p), 0.0)
                            at = k * (frames // LANES)
                            data[p][at] = data[p][at] + extra
                square = sum(a * a + b * b for a, b in zip(*data))
                power = jnp.sum(square, axis=1, keepdims=True)
                factor = lax.rsqrt(power * (1.0 / (frames * parts)) + 1.0)
                top = (c // 8) * (8 * spans) + c % 8
                for k in range(parts):
                    source = lax.rem(me + parts - k, parts) * (frames // LANES)
                    for p in range(2):
                        for u in range(frames // LANES):
                            row = pl.ds(top + (source + u) * 8, each, stride=rows * spans)
                            out_ref[s, p, row, :] = data[p][k * (frames // LANES) + u] * factor

    for s in range(streams):
        for b in reversed(range(blocks)):
            widen(s, b)
            if s > 0 and b == blocks - 2:

                @pl.when(me < parts - 1)
                def _():
                    for k in range(1, parts):
                        overhang(s, k).start()

            if b == 0:
                if s + 1 < streams:
                    for n in reversed(range(blocks)):
                        load(s + 1, n).start()
                if s == 0:

                    @pl.when(me > 0)
                    def _():
                        edge().wait_recv()
                        wide[:past] = halo[...].astype(jnp.float32)

                if s == 0:

                    @pl.when(me == 0)
                    def _():
                        wide[:past] = jnp.zeros((past, 2 * rows, LANES), jnp.float32)

                if s == 1:
                    wide[:past] = jnp.zeros((past, 2 * rows, LANES), jnp.float32)

            @pl.loop(0, SPAN // BATCH)
            def _(step):
                base = pl.multiple_of(step * BATCH, BATCH)
                first_stage(b * SPAN + base, base, SPAN + 8)

            @pl.loop(0, steps)
            def _(step):
                out = second_stage(step, quad, SPAN, SPAN + 8)
                keep(out, own.at[s, b, step], [send.at[s, k, b, step] for k in range(parts - 1)])

                @pl.when(step > 0)
                def _():
                    for k in range(1, parts):
                        piece(s, k, b, step - 1).start()

            for k in range(1, parts):
                piece(s, k, b, steps - 1).start()

            if s > 0 and b == blocks - 1:

                @pl.loop(0, over // BATCH)
                def _(step):
                    base = pl.multiple_of(step * BATCH, BATCH)
                    first_stage(frames + base, base, over + 8)

                @pl.loop(0, rows // group)
                def _(step):
                    out = second_stage(step, group, over, over + 8)
                    keep(out, own_over.at[s - 1, step],
                         [send_over.at[s - 1, k, step] for k in range(parts - 1)])

    for s in range(streams):
        if s > 0:
            for k in range(1, parts):

                @pl.when(lax.rem(me + parts - k, parts) < parts - 1)
                def _():
                    overhang(s, k).wait_recv()

        @pl.loop(0, steps)
        def _(step):
            finish(s, step)

    for s in range(streams):

        @pl.loop(0, steps)
        def _(step):
            for k in range(1, parts):
                for b in range(blocks):
                    piece(s, k, b, step).wait_send()

    @pl.when(me < parts - 1)
    def _():
        edge().wait_send()
        for s in range(1, streams):
            for k in range(1, parts):
                overhang(s, k).wait_send()


def shards(parts, signal, taps):
    streams = signal.shape[0]
    depth, channels = taps.shape
    rows = channels // LANES
    frames = signal.shape[2] // channels
    each = LANES // parts
    chunks = signal.shape[2] // LANES
    x = signal.reshape(streams, 2, chunks, LANES).transpose(0, 2, 1, 3)
    x = x.reshape(streams, frames, 2 * rows, LANES)
    taps = taps.reshape(depth // 8, 8, rows, LANES).transpose(0, 2, 1, 3)
    twist = angles(rows, LANES, channels)
    cos, sin = jnp.asarray(np.cos(twist), jnp.float32), jnp.asarray(np.sin(twist), jnp.float32)
    first = jnp.asarray(first_table(rows))
    second = jnp.asarray(second_table(channels, parts))
    blocks = frames // SPAN
    steps = rows * SPAN // WIDE
    over = -(-(depth - 1) // BATCH) * BATCH
    pitch = SPAN + 8
    reach = 2 * rows + 8
    spans = frames * parts // LANES
    tiles = channels // parts // 8
    width = 2 * rows * LANES * frames
    limit = (8 << 20) + 2 * width + 4 * width + 4 * width * 9 // 8 + 8 * width * streams * (parts + 1) // parts
    hbm = pl.BlockSpec(memory_space=pltpu.HBM)
    code = (streams, parts - 1, blocks, steps, WIDE // LANES, 2, each, LANES)
    hung = (streams - 1, parts - 1, rows * over // WIDE, WIDE // LANES, 2, each, LANES)
    operands = [x, taps, first, cos, sin, second]
    operands = [pltpu.with_memory_space_constraint(a, pltpu.HBM) for a in operands]
    out = pl.pallas_call(
        functools.partial(channelize, parts, streams, frames, rows, depth),
        in_specs=[hbm] * 6,
        out_specs=pl.BlockSpec(memory_space=pltpu.VMEM),
        out_shape=pltpu.VMEM((streams, 2, 8 * tiles * spans, LANES), jnp.float32),
        scratch_shapes=[
            pltpu.VMEM((frames, 2 * rows, LANES), jnp.bfloat16),
            pltpu.VMEM(taps.shape, jnp.float32),
            pltpu.VMEM((depth * reach, LANES), jnp.float32),
            pltpu.VMEM(first.shape, jnp.bfloat16),
            pltpu.VMEM(cos.shape, jnp.float32),
            pltpu.VMEM(sin.shape, jnp.float32),
            pltpu.VMEM(second.shape, jnp.bfloat16),
            pltpu.VMEM((depth - 1, 2 * rows, LANES), jnp.bfloat16),
            pltpu.VMEM((depth - 1 + frames + over, 2 * rows, LANES), jnp.float32),
            pltpu.VMEM((2 * GROUP * rows, 2 * LANES), jnp.float32),
            pltpu.VMEM((rows * pitch, LANES), jnp.float32),
            pltpu.VMEM((rows * pitch, LANES), jnp.float32),
            pltpu.VMEM(code[:1] + code[2:], jnp.float32),
            pltpu.VMEM(code, jnp.bfloat16),
            pltpu.VMEM(code, jnp.bfloat16),
            pltpu.VMEM(hung[:1] + hung[2:], jnp.float32),
            pltpu.VMEM(hung, jnp.bfloat16),
            pltpu.VMEM(hung, jnp.bfloat16),
            pltpu.SemaphoreType.DMA((blocks,)),
            pltpu.SemaphoreType.DMA((5,)),
            pltpu.SemaphoreType.DMA,
            pltpu.SemaphoreType.DMA,
            pltpu.SemaphoreType.DMA(code[:4]),
            pltpu.SemaphoreType.DMA(code[:4]),
            pltpu.SemaphoreType.DMA(hung[:2]),
            pltpu.SemaphoreType.DMA(hung[:2]),
        ],
        compiler_params=pltpu.CompilerParams(
            vmem_limit_bytes=limit, collective_id=0, has_side_effects=True),
        cost_estimate=pl.CostEstimate(flops=16 * 10**9, bytes_accessed=16 << 20, transcendentals=0),
        name="channelize",
    )(*operands)
    out = out.reshape(streams, 2, tiles, spans, 8, LANES).transpose(0, 1, 2, 4, 3, 5)
    return out.reshape(streams, 2, 8 * tiles, spans * LANES)


def solution(mesh):
    in_specs = (P("stream", None, "tm"), P())
    out_specs = P("stream", None, "tm", None)
    body = functools.partial(shards, mesh.shape["tm"])
    return jax.shard_map(body, mesh=mesh, in_specs=in_specs, out_specs=out_specs, check_vma=False)
```

```python
import functools
import math

import jax
import jax.numpy as jnp
import numpy as np
from jax import lax
from jax.experimental import pallas as pl
from jax.experimental.pallas import tpu as pltpu
from jax.sharding import PartitionSpec as P

LANES = 128
GROUP = 4
BATCH = 2 * GROUP
SPAN = 64
WIDE = 2 * LANES
POWER = 6
SCALE = 64.0


def angles(height, breadth, modulus):
    product = np.arange(height)[:, None] * np.arange(breadth)[None, :] % modulus
    return product * (2.0 * math.pi / modulus)


def split(table):
    high = table.astype(np.float32).astype(jnp.bfloat16)
    low = (table - high.astype(np.float64)).astype(np.float32).astype(jnp.bfloat16)
    return high, low


def first_table(rows):
    turn = angles(rows, rows, rows)
    cos, sin = np.cos(turn), np.sin(turn)
    whole = np.block([[cos, sin], [-sin, cos]])
    woven = whole.reshape(2 * rows, 2, rows).transpose(0, 2, 1).reshape(2 * rows, 2 * rows)
    high, low = split(np.kron(np.eye(GROUP), woven))
    return np.concatenate([high, low, high], axis=1)


def second_table(channels, parts):
    turn = angles(LANES, LANES, LANES)
    scale = 1.0 / math.isqrt(channels)
    cos, sin = np.cos(turn) * scale, np.sin(turn) * scale
    each = LANES // parts
    blocks = []
    for part in range(parts):
        pick = slice(part * each, (part + 1) * each)
        blocks.append(np.block([[cos[pick], sin[pick]], [-sin[pick], cos[pick]]]))
    high, low = split(np.concatenate(blocks, axis=0))
    table = np.concatenate([high, low, high], axis=1)
    return np.concatenate([table, table], axis=0)


def encode(value):
    value = value * SCALE
    square = value * jnp.abs(value)
    return (square * (square * square)).astype(jnp.bfloat16)


def decode(code):
    value = code.astype(jnp.float32)
    size = jnp.exp(jnp.log(jnp.abs(value)) * (1.0 / POWER)) * (1.0 / SCALE)
    return jnp.where(value < 0.0, -size, size)


def halves(value):
    high = value.astype(jnp.bfloat16)
    low = (value - high.astype(jnp.float32)).astype(jnp.bfloat16)
    return high, low


def equalize(parts, s, step, own, recv, own_over, recv_over, put):
    me = lax.axis_index("tm")
    blocks, each = own.shape[1], own.shape[5]
    spans = blocks * SPAN // LANES
    quad = WIDE // SPAN
    group = own.shape[2] * quad // own_over.shape[1]
    over = WIDE // group
    lanes = lax.broadcasted_iota(jnp.int32, (each, LANES), 1)
    left = lanes < SPAN

    def fetch(k, b, j, p):
        if k == 0:
            return own[s, b, step, j, p]
        return decode(recv[s, k - 1, b, step, j, p])

    def hung(k, c, p):
        at, slot = c // group, (c % group) // (LANES // over)
        if k == 0:
            value = own_over[s - 1, at, slot, p]
        else:
            value = decode(recv_over[s - 1, k - 1, at, slot, p])
        turn = lax.rem(LANES - (c % (LANES // over)) * over, LANES)
        return jnp.where(lanes < over, pltpu.roll(value, turn, 1), 0.0)

    for j in range(WIDE // LANES):
        whole = [[[], []] for _ in range(LANES // SPAN)]
        for k in range(parts):
            for p in range(2):
                for u in range(spans):
                    low, high = fetch(k, 2 * u, j, p), fetch(k, 2 * u + 1, j, p)
                    whole[0][p].append(jnp.where(left, low, pltpu.roll(high, SPAN, 1)))
                    whole[1][p].append(jnp.where(left, pltpu.roll(low, SPAN, 1), high))
        for i in range(LANES // SPAN):
            c = step * quad + j * (LANES // SPAN) + i
            data = whole[i]
            if s > 0:
                for k in range(parts):
                    source = lax.rem(me + parts - k, parts)
                    for p in range(2):
                        extra = jnp.where(source > 0, hung((k + 1) % parts, c, p), 0.0)
                        data[p][k * spans] = data[p][k * spans] + extra
            square = sum(a * a + b * b for a, b in zip(*data))
            power = jnp.sum(square, axis=1, keepdims=True)
            factor = lax.rsqrt(power * (1.0 / (parts * spans * LANES)) + 1.0)
            for k in range(parts):
                source = lax.rem(me + parts - k, parts) * spans
                for p in range(2):
                    for u in range(spans):
                        put(p, c, source + u, data[p][k * spans + u] * factor)


def channelize(parts, streams, frames, rows, depth, x_hbm, taps_hbm, first_hbm, cos_hbm, sin_hbm,
               second_hbm, out_ref, own, recv, own_over, recv_over, xbuf, taps_raw, taps_ref,
               first_ref, cos_ref, sin_ref, second_ref, halo, wide, grid, zr, zi, send, send_over,
               x_sem, table_sem, halo_send, halo_recv, send_sem, recv_sem, over_send, over_recv):
    me = lax.axis_index("tm")
    each = LANES // parts
    past = depth - 1
    over = -(-past // BATCH) * BATCH
    blocks = frames // SPAN
    quad = WIDE // SPAN
    steps = rows // quad
    group = WIDE // over
    spans = frames * parts // LANES
    reach = taps_ref.shape[0] // depth
    bounds = [max(b * SPAN - over, 0) for b in range(blocks)] + [frames]

    barrier = pltpu.get_barrier_semaphore()
    for k in range(1, parts):
        pl.semaphore_signal(barrier, inc=1, device_id={"tm": lax.rem(me + k, parts)},
                            device_id_type=pl.DeviceIdType.MESH)

    def load(s, b):
        pick = pl.ds(bounds[b], bounds[b + 1] - bounds[b])
        return pltpu.make_async_copy(x_hbm.at[s, pick], xbuf.at[pick], x_sem.at[b])

    def edge():
        return pltpu.make_async_remote_copy(
            src_ref=x_hbm.at[0, pl.ds(frames - past, past)], dst_ref=halo,
            send_sem=halo_send, recv_sem=halo_recv,
            device_id={"tm": lax.rem(me + 1, parts)}, device_id_type=pl.DeviceIdType.MESH)

    def piece(s, k, b, step):
        return pltpu.make_async_remote_copy(
            src_ref=send.at[s, k - 1, b, step], dst_ref=recv.at[s, k - 1, b, step],
            send_sem=send_sem.at[s, k - 1, b, step], recv_sem=recv_sem.at[s, k - 1, b, step],
            device_id={"tm": lax.rem(me + k, parts)}, device_id_type=pl.DeviceIdType.MESH)

    def overhang(s, k):
        return pltpu.make_async_remote_copy(
            src_ref=send_over.at[s - 1, k - 1], dst_ref=recv_over.at[s - 1, k - 1],
            send_sem=over_send.at[s - 1, k - 1], recv_sem=over_recv.at[s - 1, k - 1],
            device_id={"tm": lax.rem(me + k, parts)}, device_id_type=pl.DeviceIdType.MESH)

    load(0, blocks - 1).start()
    tables = [
        pltpu.make_async_copy(source, target, table_sem.at[i])
        for i, (source, target) in enumerate([
            (taps_hbm, taps_raw), (first_hbm, first_ref), (cos_hbm, cos_ref),
            (sin_hbm, sin_ref), (second_hbm, second_ref)])
    ]
    for table in tables:
        table.start()
    for b in reversed(range(blocks - 1)):
        load(0, b).start()
    pl.semaphore_wait(barrier, parts - 1)

    @pl.when(me < parts - 1)
    def _():
        edge().start()

    for table in tables:
        table.wait()

    @pl.loop(0, rows)
    def _(n):
        for g in range(depth // 8):
            for p in range(2):
                row = pl.ds(g * 8 * reach + 2 * n + p, 8, stride=reach)
                taps_ref[row, :] = taps_raw[g, n]

    wide[past + frames :] = jnp.zeros((over, 2 * rows, LANES), jnp.float32)

    def widen(s, b):
        load(s, b).wait()

        @pl.loop(bounds[b] // BATCH, bounds[b + 1] // BATCH)
        def _(step):
            base = pl.multiple_of(step * BATCH, BATCH)
            wide[pl.ds(base + past, BATCH)] = xbuf[pl.ds(base, BATCH)].astype(jnp.float32)

    def first_stage(frame, slot, pitch):
        for block in range(2 * rows // 8):
            sub = slice(block * 8, block * 8 + 8)
            data = [wide[frame + i, sub, :] for i in range(BATCH + past)]
            taps = [taps_ref[k * reach + block * 8 : k * reach + block * 8 + 8, :]
                    for k in range(depth)]
            for t in range(BATCH):
                total = taps[0] * data[t + past]
                for k in range(1, depth):
                    total = total + taps[k] * data[t + past - k]
                row = (t % GROUP) * 2 * rows + block * 8
                lane = (t // GROUP) * LANES
                grid[row : row + 8, lane : lane + LANES] = total
        high, low = halves(grid[...])
        out = jnp.dot(first_ref[...], jnp.concatenate([high, high, low], axis=0),
                      preferred_element_type=jnp.float32)
        cos, sin = cos_ref[...], sin_ref[...]
        for t in range(BATCH):
            row = (t % GROUP) * 2 * rows
            lane = (t // GROUP) * LANES
            real = out[row : row + rows, lane : lane + LANES]
            imag = out[row + rows : row + 2 * rows, lane : lane + LANES]
            pick = pl.ds(slot + t, rows, stride=pitch)
            zr[pick, :] = real * cos + imag * sin
            zi[pick, :] = imag * cos - real * sin

    def second_stage(step, count, length, pitch):
        pieces = []
        for i in range(count):
            pick = pl.ds(pl.multiple_of((step * count + i) * pitch, 8), length)
            pieces.append(jnp.concatenate([zr[pick, :], zi[pick, :]], axis=1))
        high, low = halves(jnp.concatenate(pieces, axis=0))
        top = pl.ds(pl.multiple_of(me * 2 * each, 2 * each), 2 * LANES)
        return lax.dot_general(second_ref[top, :], jnp.concatenate([high, high, low], axis=1),
                               (((1,), (1,)), ((), ())), preferred_element_type=jnp.float32)

    def keep(out, mine, theirs):
        for j in range(WIDE // LANES):
            lane = slice(j * LANES, (j + 1) * LANES)
            for p in range(2):
                mine[j, p] = out[p * each : (p + 1) * each, lane]
                for k in range(1, parts):
                    row = (2 * k + p) * each
                    theirs[k - 1][j, p] = encode(out[row : row + each, lane])

    def finish(s, step):
        for k in range(1, parts):
            for b in range(blocks):
                piece(s, k, b, step).wait_recv()
        pitch = out_ref.shape[2] // each

        def put(p, c, span, value):
            row = pl.ds((c // 8) * (8 * spans) + span * 8 + c % 8, each, stride=pitch)
            out_ref[s, p, row, :] = value

        equalize(parts, s, step, own, recv, own_over, recv_over, put)

    for s in range(streams):
        for b in reversed(range(blocks)):
            widen(s, b)
            if s > 0 and b == blocks - 2:

                @pl.when(me < parts - 1)
                def _():
                    for k in range(1, parts):
                        overhang(s, k).start()

            if b == 0:
                if s + 1 < streams:
                    for n in reversed(range(blocks)):
                        load(s + 1, n).start()
                if s == 0:

                    @pl.when(me > 0)
                    def _():
                        edge().wait_recv()
                        wide[:past] = halo[...].astype(jnp.float32)

                if s == 0:

                    @pl.when(me == 0)
                    def _():
                        wide[:past] = jnp.zeros((past, 2 * rows, LANES), jnp.float32)

                if s == 1:
                    wide[:past] = jnp.zeros((past, 2 * rows, LANES), jnp.float32)

            @pl.loop(0, SPAN // BATCH)
            def _(step):
                base = pl.multiple_of(step * BATCH, BATCH)
                first_stage(b * SPAN + base, base, SPAN + 8)

            @pl.loop(0, steps)
            def _(step):
                out = second_stage(step, quad, SPAN, SPAN + 8)
                keep(out, own.at[s, b, step], [send.at[s, k, b, step] for k in range(parts - 1)])

                @pl.when(step > 0)
                def _():
                    for k in range(1, parts):
                        piece(s, k, b, step - 1).start()

            for k in range(1, parts):
                piece(s, k, b, steps - 1).start()

            if s > 0 and b == blocks - 1:

                @pl.loop(0, over // BATCH)
                def _(step):
                    base = pl.multiple_of(step * BATCH, BATCH)
                    first_stage(frames + base, base, over + 8)

                @pl.loop(0, rows // group)
                def _(step):
                    out = second_stage(step, group, over, over + 8)
                    keep(out, own_over.at[s - 1, step],
                         [send_over.at[s - 1, k, step] for k in range(parts - 1)])

    for s in range(streams):
        if s > 0:
            for k in range(1, parts):

                @pl.when(lax.rem(me + parts - k, parts) < parts - 1)
                def _():
                    overhang(s, k).wait_recv()

        early = steps if s + 1 < streams else steps - 8 // quad

        @pl.loop(0, early)
        def _(step):
            finish(s, step)

        @pl.loop(early, steps)
        def _(step):
            for k in range(1, parts):
                for b in range(blocks):
                    piece(s, k, b, step).wait_recv()

    for s in range(streams):

        @pl.loop(0, steps)
        def _(step):
            for k in range(1, parts):
                for b in range(blocks):
                    piece(s, k, b, step).wait_send()

    @pl.when(me < parts - 1)
    def _():
        edge().wait_send()
        for s in range(1, streams):
            for k in range(1, parts):
                overhang(s, k).wait_send()


def deliver(parts, planes, own, recv, own_over, recv_over, out_ref, tail, plane_sem, tail_sem):
    streams, each = own.shape[0], own.shape[5]
    rows = out_ref.shape[3]
    steps, quad = own.shape[2], WIDE // SPAN
    last = streams - 1
    spans = rows // (steps * quad)
    ready = rows - 8 * spans
    pitch = tail.shape[1] // each
    copies = []
    for s in range(streams):
        for p in range(2):
            pick = pl.ds(0, rows if s < last else ready)
            copies.append(pltpu.make_async_copy(
                planes.at[s, p, :, pick], out_ref.at[s, p, :, pick], plane_sem.at[s, p]))
    for copy in copies:
        copy.start()

    def put(p, c, span, value):
        tail[p, pl.ds(span * 8 + c % 8, each, stride=pitch), :] = value

    @pl.loop(steps - 8 // quad, steps)
    def _(step):
        equalize(parts, last, step, own, recv, own_over, recv_over, put)

    for p in range(2):
        source = tail.at[p].reshape(each, pitch, LANES).at[:, pl.ds(0, 8 * spans)]
        copies.append(pltpu.make_async_copy(
            source, out_ref.at[last, p, :, pl.ds(ready, 8 * spans)], tail_sem.at[p]))
    for copy in copies[-2:]:
        copy.start()
    for copy in copies:
        copy.wait()


def shards(parts, signal, taps):
    streams = signal.shape[0]
    depth, channels = taps.shape
    rows = channels // LANES
    frames = signal.shape[2] // channels
    each = LANES // parts
    chunks = signal.shape[2] // LANES
    x = signal.reshape(streams, 2, chunks, LANES).transpose(0, 2, 1, 3)
    x = x.reshape(streams, frames, 2 * rows, LANES)
    taps = taps.reshape(depth // 8, 8, rows, LANES).transpose(0, 2, 1, 3)
    twist = angles(rows, LANES, channels)
    cos, sin = jnp.asarray(np.cos(twist), jnp.float32), jnp.asarray(np.sin(twist), jnp.float32)
    first = jnp.asarray(first_table(rows))
    second = jnp.asarray(second_table(channels, parts))
    blocks = frames // SPAN
    steps = rows * SPAN // WIDE
    over = -(-(depth - 1) // BATCH) * BATCH
    pitch = SPAN + 8
    reach = 2 * rows + 8
    spans = frames * parts // LANES
    tiles = channels // parts // 8
    width = 2 * rows * LANES * frames
    limit = (8 << 20) + 2 * width + 4 * width + 4 * width * 9 // 8 + 8 * width * streams * (parts + 1) // parts
    hbm = pl.BlockSpec(memory_space=pltpu.HBM)
    code = (streams, parts - 1, blocks, steps, WIDE // LANES, 2, each, LANES)
    hung = (streams - 1, parts - 1, rows * over // WIDE, WIDE // LANES, 2, each, LANES)
    operands = [x, taps, first, cos, sin, second]
    operands = [pltpu.with_memory_space_constraint(a, pltpu.HBM) for a in operands]
    far = rows * spans + 8
    vmem = pl.BlockSpec(memory_space=pltpu.VMEM)
    kept = pl.pallas_call(
        functools.partial(channelize, parts, streams, frames, rows, depth),
        in_specs=[hbm] * 6,
        out_specs=[vmem] * 5,
        out_shape=[
            pltpu.VMEM((streams, 2, each * far, LANES), jnp.float32),
            pltpu.VMEM(code[:1] + code[2:], jnp.float32),
            pltpu.VMEM(code, jnp.bfloat16),
            pltpu.VMEM(hung[:1] + hung[2:], jnp.float32),
            pltpu.VMEM(hung, jnp.bfloat16),
        ],
        scratch_shapes=[
            pltpu.VMEM((frames, 2 * rows, LANES), jnp.bfloat16),
            pltpu.VMEM(taps.shape, jnp.float32),
            pltpu.VMEM((depth * reach, LANES), jnp.float32),
            pltpu.VMEM(first.shape, jnp.bfloat16),
            pltpu.VMEM(cos.shape, jnp.float32),
            pltpu.VMEM(sin.shape, jnp.float32),
            pltpu.VMEM(second.shape, jnp.bfloat16),
            pltpu.VMEM((depth - 1, 2 * rows, LANES), jnp.bfloat16),
            pltpu.VMEM((depth - 1 + frames + over, 2 * rows, LANES), jnp.float32),
            pltpu.VMEM((2 * GROUP * rows, 2 * LANES), jnp.float32),
            pltpu.VMEM((rows * pitch, LANES), jnp.float32),
            pltpu.VMEM((rows * pitch, LANES), jnp.float32),
            pltpu.VMEM(code, jnp.bfloat16),
            pltpu.VMEM(hung, jnp.bfloat16),
            pltpu.SemaphoreType.DMA((blocks,)),
            pltpu.SemaphoreType.DMA((5,)),
            pltpu.SemaphoreType.DMA,
            pltpu.SemaphoreType.DMA,
            pltpu.SemaphoreType.DMA(code[:4]),
            pltpu.SemaphoreType.DMA(code[:4]),
            pltpu.SemaphoreType.DMA(hung[:2]),
            pltpu.SemaphoreType.DMA(hung[:2]),
        ],
        compiler_params=pltpu.CompilerParams(
            vmem_limit_bytes=limit, collective_id=0, has_side_effects=True),
        cost_estimate=pl.CostEstimate(flops=16 * 10**9, bytes_accessed=16 << 20, transcendentals=0),
        name="channelize",
    )(*operands)
    kept = [kept[0].reshape(streams, 2, each, far, LANES), *kept[1:]]
    kept = [pltpu.with_memory_space_constraint(a, pltpu.VMEM) for a in kept]
    out = pl.pallas_call(
        functools.partial(deliver, parts),
        in_specs=[vmem] * 5,
        out_specs=hbm,
        out_shape=jax.ShapeDtypeStruct((streams, 2, each, rows * spans, LANES), jnp.float32),
        scratch_shapes=[
            pltpu.VMEM((2, each * (8 * spans + 8), LANES), jnp.float32),
            pltpu.SemaphoreType.DMA((streams, 2)),
            pltpu.SemaphoreType.DMA((2,)),
        ],
        compiler_params=pltpu.CompilerParams(vmem_limit_bytes=limit),
        cost_estimate=pl.CostEstimate(flops=10**7, bytes_accessed=16 << 20, transcendentals=0),
        name="deliver",
    )(*kept)
    out = out.reshape(streams, 2, tiles, spans, 8, LANES).transpose(0, 1, 2, 4, 3, 5)
    return out.reshape(streams, 2, 8 * tiles, spans * LANES)


def solution(mesh):
    in_specs = (P("stream", None, "tm"), P())
    out_specs = P("stream", None, "tm", None)
    body = functools.partial(shards, mesh.shape["tm"])
    return jax.shard_map(body, mesh=mesh, in_specs=in_specs, out_specs=out_specs, check_vma=False)
```

```python
import functools
import math

import jax
import jax.numpy as jnp
import numpy as np
from jax import lax
from jax.experimental import pallas as pl
from jax.experimental.pallas import tpu as pltpu
from jax.sharding import PartitionSpec as P

LANES = 128
GROUP = 4
BATCH = 2 * GROUP
SPAN = 32
CHUNK = 16
WIDE = 2 * LANES
POWER = 6
SCALE = 64.0


def angles(height, breadth, modulus):
    product = np.arange(height)[:, None] * np.arange(breadth)[None, :] % modulus
    return product * (2.0 * math.pi / modulus)


def split(table):
    high = table.astype(np.float32).astype(jnp.bfloat16)
    low = (table - high.astype(np.float64)).astype(np.float32).astype(jnp.bfloat16)
    return high, low


def first_table(rows):
    turn = angles(rows, rows, rows)
    cos, sin = np.cos(turn), np.sin(turn)
    whole = np.block([[cos, sin], [-sin, cos]])
    woven = whole.reshape(2 * rows, 2, rows).transpose(0, 2, 1).reshape(2 * rows, 2 * rows)
    high, low = split(np.kron(np.eye(GROUP), woven))
    return np.concatenate([high, low, high], axis=1)


def second_table(channels, parts):
    turn = angles(LANES, LANES, LANES)
    scale = 1.0 / math.isqrt(channels)
    cos, sin = np.cos(turn) * scale, np.sin(turn) * scale
    each = LANES // parts
    blocks = []
    for part in range(parts):
        pick = slice(part * each, (part + 1) * each)
        blocks.append(np.block([[cos[pick], sin[pick]], [-sin[pick], cos[pick]]]))
    high, low = split(np.concatenate(blocks, axis=0))
    table = np.concatenate([high, low, high], axis=1)
    return np.concatenate([table, table], axis=0)


def encode(value):
    value = value * SCALE
    square = value * jnp.abs(value)
    return (square * (square * square)).astype(jnp.bfloat16)


def decode(code):
    value = code.astype(jnp.float32)
    size = jnp.exp(jnp.log(jnp.abs(value)) * (1.0 / POWER)) * (1.0 / SCALE)
    return jnp.where(value < 0.0, -size, size)


def halves(value):
    high = value.astype(jnp.bfloat16)
    low = (value - high.astype(jnp.float32)).astype(jnp.bfloat16)
    return high, low


def equalize(parts, s, step, own, recv, own_over, recv_over, put):
    me = lax.axis_index("tm")
    blocks, each = own.shape[1], own.shape[5]
    fold = LANES // SPAN
    spans = blocks // fold
    quad = WIDE // SPAN
    group = own.shape[2] * quad // own_over.shape[1]
    over = WIDE // group
    lanes = lax.broadcasted_iota(jnp.int32, (CHUNK, LANES), 1)
    segment = lanes // SPAN
    sources = [lax.rem(me + parts - k, parts) for k in range(parts)]

    def move(value, shift):
        return pltpu.roll(value, shift % LANES, 1) if shift % LANES else value

    for r in range(0, each, CHUNK):
        sub = slice(r, r + CHUNK)

        def fetch(k, b, j, p):
            if k == 0:
                return own[s, b, step, j, p, sub]
            return decode(recv[s, k - 1, b, step, j, p, sub])

        def hung(k, p):
            at, slot = step * quad // group, step * quad % group // (LANES // over)
            if k == 0:
                return own_over[s - 1, at, slot, p, sub]
            return decode(recv_over[s - 1, k - 1, at, slot, p, sub])

        if s > 0:
            extras = [[jnp.where(sources[k] > 0, hung((k + 1) % parts, p), 0.0)
                       for p in range(2)] for k in range(parts)]

        for j in range(WIDE // LANES):
            tiles = [[[fetch(k, b, j, p) for b in range(blocks)] for p in range(2)]
                     for k in range(parts)]
            for i in range(fold):
                n = j * fold + i
                data = [[], []]
                for k in range(parts):
                    for p in range(2):
                        for u in range(spans):
                            value = tiles[k][p][u * fold]
                            for q in range(1, fold):
                                here = segment == (i + q) % fold
                                value = jnp.where(here, tiles[k][p][u * fold + q], value)
                            if s > 0 and u == 0:
                                extra = move(extras[k][p], -j * over)
                                inside = (segment == i) & (lanes % SPAN < over)
                                value = value + jnp.where(inside, extra, 0.0)
                            data[p].append(move(value, -i * SPAN))
                square = sum(a * a + b * b for a, b in zip(*data))
                power = jnp.sum(square, axis=1, keepdims=True)
                factor = lax.rsqrt(power * (1.0 / (parts * spans * LANES)) + 1.0)
                for k in range(parts):
                    for p in range(2):
                        for u in range(spans):
                            put(p, step * quad + n, n, sources[k] * spans + u, r,
                                data[p][k * spans + u] * factor)


def channelize(parts, streams, frames, rows, depth, x_hbm, taps_hbm, first_hbm, cos_hbm, sin_hbm,
               second_hbm, out_ref, own, recv, own_over, recv_over, xbuf, taps_raw, taps_ref,
               first_ref, cos_ref, sin_ref, second_ref, halo, wide, grid, zr, zi, send, send_over,
               x_sem, table_sem, halo_send, halo_recv, send_sem, recv_sem, over_send, over_recv):
    me = lax.axis_index("tm")
    each = LANES // parts
    past = depth - 1
    over = -(-past // BATCH) * BATCH
    blocks = frames // SPAN
    quad = WIDE // SPAN
    fold = LANES // SPAN
    steps = rows // quad
    group = WIDE // over
    spans = frames * parts // LANES
    reach = taps_ref.shape[0] // depth
    bounds = [max(b * SPAN - over, 0) for b in range(blocks)] + [frames]

    barrier = pltpu.get_barrier_semaphore()
    for k in range(1, parts):
        pl.semaphore_signal(barrier, inc=1, device_id={"tm": lax.rem(me + k, parts)},
                            device_id_type=pl.DeviceIdType.MESH)

    def load(s, b):
        pick = pl.ds(bounds[b], bounds[b + 1] - bounds[b])
        return pltpu.make_async_copy(x_hbm.at[s, pick], xbuf.at[pick], x_sem.at[b])

    def edge():
        return pltpu.make_async_remote_copy(
            src_ref=x_hbm.at[0, pl.ds(frames - past, past)], dst_ref=halo,
            send_sem=halo_send, recv_sem=halo_recv,
            device_id={"tm": lax.rem(me + 1, parts)}, device_id_type=pl.DeviceIdType.MESH)

    def piece(s, k, b, step):
        return pltpu.make_async_remote_copy(
            src_ref=send.at[s, k - 1, b, step], dst_ref=recv.at[s, k - 1, b, step],
            send_sem=send_sem.at[s, k - 1, b, step], recv_sem=recv_sem.at[s, k - 1, b, step],
            device_id={"tm": lax.rem(me + k, parts)}, device_id_type=pl.DeviceIdType.MESH)

    def overhang(s, k):
        return pltpu.make_async_remote_copy(
            src_ref=send_over.at[s - 1, k - 1], dst_ref=recv_over.at[s - 1, k - 1],
            send_sem=over_send.at[s - 1, k - 1], recv_sem=over_recv.at[s - 1, k - 1],
            device_id={"tm": lax.rem(me + k, parts)}, device_id_type=pl.DeviceIdType.MESH)

    load(0, blocks - 1).start()
    tables = [
        pltpu.make_async_copy(source, target, table_sem.at[i])
        for i, (source, target) in enumerate([
            (taps_hbm, taps_raw), (first_hbm, first_ref), (cos_hbm, cos_ref),
            (sin_hbm, sin_ref), (second_hbm, second_ref)])
    ]
    for table in tables:
        table.start()
    pl.semaphore_wait(barrier, parts - 1)

    @pl.when(me < parts - 1)
    def _():
        edge().start()

    for b in reversed(range(blocks - 1)):
        load(0, b).start()
    tables[0].wait()

    @pl.loop(0, rows)
    def _(n):
        for g in range(depth // 8):
            for p in range(2):
                row = pl.ds(g * 8 * reach + 2 * n + p, 8, stride=reach)
                taps_ref[row, :] = taps_raw[g, n]

    def widen(s, b):
        load(s, b).wait()

        @pl.loop(bounds[b] // BATCH, bounds[b + 1] // BATCH)
        def _(step):
            base = pl.multiple_of(step * BATCH, BATCH)
            wide[pl.ds(base + past, BATCH)] = xbuf[pl.ds(base, BATCH)].astype(jnp.float32)

    def first_stage(frame, slot, pitch):
        for block in range(2 * rows // 8):
            sub = slice(block * 8, block * 8 + 8)
            data = [wide[frame + i, sub, :] for i in range(BATCH + past)]
            taps = [taps_ref[k * reach + block * 8 : k * reach + block * 8 + 8, :]
                    for k in range(depth)]
            for t in range(BATCH):
                total = taps[0] * data[t + past]
                for k in range(1, depth):
                    total = total + taps[k] * data[t + past - k]
                row = (t % GROUP) * 2 * rows + block * 8
                lane = (t // GROUP) * LANES
                grid[row : row + 8, lane : lane + LANES] = total
        high, low = halves(grid[...])
        out = jnp.dot(first_ref[...], jnp.concatenate([high, high, low], axis=0),
                      preferred_element_type=jnp.float32)
        cos, sin = cos_ref[...], sin_ref[...]
        for t in range(BATCH):
            row = (t % GROUP) * 2 * rows
            lane = (t // GROUP) * LANES
            real = out[row : row + rows, lane : lane + LANES]
            imag = out[row + rows : row + 2 * rows, lane : lane + LANES]
            pick = pl.ds(slot + t, rows, stride=pitch)
            zr[pick, :] = real * cos + imag * sin
            zi[pick, :] = imag * cos - real * sin

    def second_stage(step, order, length, pitch):
        pieces = []
        for i in order:
            pick = pl.ds(pl.multiple_of((step * len(order) + i) * pitch, 8), length)
            pieces.append(jnp.concatenate([zr[pick, :], zi[pick, :]], axis=1))
        high, low = halves(jnp.concatenate(pieces, axis=0))
        top = pl.ds(pl.multiple_of(me * 2 * each, 2 * each), 2 * LANES)
        return lax.dot_general(second_ref[top, :], jnp.concatenate([high, high, low], axis=1),
                               (((1,), (1,)), ((), ())), preferred_element_type=jnp.float32)

    def keep(out, mine, theirs):
        for j in range(WIDE // LANES):
            lane = slice(j * LANES, (j + 1) * LANES)
            for p in range(2):
                mine[j, p] = out[p * each : (p + 1) * each, lane]
                for k in range(1, parts):
                    row = (2 * k + p) * each
                    theirs[k - 1][j, p] = encode(out[row : row + each, lane])

    def finish(s, step):
        for k in range(1, parts):
            for b in range(blocks):
                piece(s, k, b, step).wait_recv()
        pitch = out_ref.shape[2] // each

        def put(p, c, n, span, r, value):
            top = (c // 8) * (8 * spans) + span * 8 + n % 8
            out_ref[s, p, pl.ds(top + r * pitch, CHUNK, stride=pitch), :] = value

        equalize(parts, s, step, own, recv, own_over, recv_over, put)

    for s in range(streams):
        for b in reversed(range(blocks)):
            widen(s, b)
            if s > 0 and b == blocks - 2:

                @pl.when(me < parts - 1)
                def _():
                    for k in range(1, parts):
                        overhang(s, k).start()

            if b == 0:
                if s + 1 < streams:
                    for n in reversed(range(blocks)):
                        load(s + 1, n).start()
                if s == 0:

                    @pl.when(me > 0)
                    def _():
                        edge().wait_recv()
                        wide[:past] = halo[...].astype(jnp.float32)

                if s == 0:

                    @pl.when(me == 0)
                    def _():
                        wide[:past] = jnp.zeros((past, 2 * rows, LANES), jnp.float32)

                if s == 1:
                    wide[:past] = jnp.zeros((past, 2 * rows, LANES), jnp.float32)

            if s == 0 and b == blocks - 1:
                for table in tables[1:4]:
                    table.wait()

            @pl.loop(0, SPAN // BATCH)
            def _(step):
                base = pl.multiple_of(step * BATCH, BATCH)
                first_stage(b * SPAN + base, base, SPAN + 8)

            if s == 0 and b == blocks - 1:
                tables[4].wait()

            @pl.loop(0, steps)
            def _(step):
                order = [j + (i - b) % fold for j in range(0, quad, fold) for i in range(fold)]
                out = second_stage(step, order, SPAN, SPAN + 8)
                keep(out, own.at[s, b, step], [send.at[s, k, b, step] for k in range(parts - 1)])

                @pl.when(step > 0)
                def _():
                    for k in range(1, parts):
                        piece(s, k, b, step - 1).start()

            for k in range(1, parts):
                piece(s, k, b, steps - 1).start()

            if s == 1 and b == blocks - 1:
                wide[past + frames :] = jnp.zeros((over, 2 * rows, LANES), jnp.float32)

            if s > 0 and b == blocks - 1:

                @pl.loop(0, over // BATCH)
                def _(step):
                    base = pl.multiple_of(step * BATCH, BATCH)
                    first_stage(frames + base, base, over + 8)

                @pl.loop(0, rows // group)
                def _(step):
                    order = [j + i % 2 * fold + i // 2
                             for j in range(0, group, 2 * fold) for i in range(2 * fold)]
                    out = second_stage(step, order, over, over + 8)
                    keep(out, own_over.at[s - 1, step],
                         [send_over.at[s - 1, k, step] for k in range(parts - 1)])

    for s in range(streams):
        if s > 0:
            for k in range(1, parts):

                @pl.when(lax.rem(me + parts - k, parts) < parts - 1)
                def _():
                    overhang(s, k).wait_recv()

        early = steps if s + 1 < streams else steps - 8 // quad

        @pl.loop(0, early)
        def _(step):
            finish(s, step)

        @pl.loop(early, steps)
        def _(step):
            for k in range(1, parts):
                for b in range(blocks):
                    piece(s, k, b, step).wait_recv()

    for s in range(streams):

        @pl.loop(0, steps)
        def _(step):
            for k in range(1, parts):
                for b in range(blocks):
                    piece(s, k, b, step).wait_send()

    @pl.when(me < parts - 1)
    def _():
        edge().wait_send()
        for s in range(1, streams):
            for k in range(1, parts):
                overhang(s, k).wait_send()


def deliver(parts, planes, own, recv, own_over, recv_over, out_ref, tail, plane_sem, tail_sem):
    streams, each = own.shape[0], own.shape[5]
    rows = out_ref.shape[3]
    steps, quad = own.shape[2], WIDE // SPAN
    last = streams - 1
    spans = rows // (steps * quad)
    ready = rows - 8 * spans
    pitch = tail.shape[1] // each
    copies = []
    for s in range(streams):
        for p in range(2):
            pick = pl.ds(0, rows if s < last else ready)
            copies.append(pltpu.make_async_copy(
                planes.at[s, p, :, pick], out_ref.at[s, p, :, pick], plane_sem.at[s, p]))
    for copy in copies:
        copy.start()

    def put(p, c, n, span, r, value):
        tail[p, pl.ds(span * 8 + n % 8 + r * pitch, CHUNK, stride=pitch), :] = value

    @pl.loop(steps - 8 // quad, steps)
    def _(step):
        equalize(parts, last, step, own, recv, own_over, recv_over, put)

    for p in range(2):
        source = tail.at[p].reshape(each, pitch, LANES).at[:, pl.ds(0, 8 * spans)]
        copies.append(pltpu.make_async_copy(
            source, out_ref.at[last, p, :, pl.ds(ready, 8 * spans)], tail_sem.at[p]))
    for copy in copies[-2:]:
        copy.start()
    for copy in copies:
        copy.wait()


def shards(parts, signal, taps):
    streams = signal.shape[0]
    depth, channels = taps.shape
    rows = channels // LANES
    frames = signal.shape[2] // channels
    each = LANES // parts
    chunks = signal.shape[2] // LANES
    x = signal.reshape(streams, 2, chunks, LANES).transpose(0, 2, 1, 3)
    x = x.reshape(streams, frames, 2 * rows, LANES)
    taps = taps.reshape(depth // 8, 8, rows, LANES).transpose(0, 2, 1, 3)
    twist = angles(rows, LANES, channels)
    cos, sin = jnp.asarray(np.cos(twist), jnp.float32), jnp.asarray(np.sin(twist), jnp.float32)
    first = jnp.asarray(first_table(rows))
    second = jnp.asarray(second_table(channels, parts))
    blocks = frames // SPAN
    steps = rows * SPAN // WIDE
    over = -(-(depth - 1) // BATCH) * BATCH
    pitch = SPAN + 8
    reach = 2 * rows + 8
    spans = frames * parts // LANES
    tiles = channels // parts // 8
    width = 2 * rows * LANES * frames
    limit = (8 << 20) + 2 * width + 4 * width + 4 * width * 9 // 8 + 8 * width * streams * (parts + 1) // parts
    hbm = pl.BlockSpec(memory_space=pltpu.HBM)
    code = (streams, parts - 1, blocks, steps, WIDE // LANES, 2, each, LANES)
    hung = (streams - 1, parts - 1, rows * over // WIDE, WIDE // LANES, 2, each, LANES)
    operands = [x, taps, first, cos, sin, second]
    operands = [pltpu.with_memory_space_constraint(a, pltpu.HBM) for a in operands]
    far = rows * spans + 8
    vmem = pl.BlockSpec(memory_space=pltpu.VMEM)
    kept = pl.pallas_call(
        functools.partial(channelize, parts, streams, frames, rows, depth),
        in_specs=[hbm] * 6,
        out_specs=[vmem] * 5,
        out_shape=[
            pltpu.VMEM((streams, 2, each * far, LANES), jnp.float32),
            pltpu.VMEM(code[:1] + code[2:], jnp.float32),
            pltpu.VMEM(code, jnp.bfloat16),
            pltpu.VMEM(hung[:1] + hung[2:], jnp.float32),
            pltpu.VMEM(hung, jnp.bfloat16),
        ],
        scratch_shapes=[
            pltpu.VMEM((frames, 2 * rows, LANES), jnp.bfloat16),
            pltpu.VMEM(taps.shape, jnp.float32),
            pltpu.VMEM((depth * reach, LANES), jnp.float32),
            pltpu.VMEM(first.shape, jnp.bfloat16),
            pltpu.VMEM(cos.shape, jnp.float32),
            pltpu.VMEM(sin.shape, jnp.float32),
            pltpu.VMEM(second.shape, jnp.bfloat16),
            pltpu.VMEM((depth - 1, 2 * rows, LANES), jnp.bfloat16),
            pltpu.VMEM((depth - 1 + frames + over, 2 * rows, LANES), jnp.float32),
            pltpu.VMEM((2 * GROUP * rows, 2 * LANES), jnp.float32),
            pltpu.VMEM((rows * pitch, LANES), jnp.float32),
            pltpu.VMEM((rows * pitch, LANES), jnp.float32),
            pltpu.VMEM(code, jnp.bfloat16),
            pltpu.VMEM(hung, jnp.bfloat16),
            pltpu.SemaphoreType.DMA((blocks,)),
            pltpu.SemaphoreType.DMA((5,)),
            pltpu.SemaphoreType.DMA,
            pltpu.SemaphoreType.DMA,
            pltpu.SemaphoreType.DMA(code[:4]),
            pltpu.SemaphoreType.DMA(code[:4]),
            pltpu.SemaphoreType.DMA(hung[:2]),
            pltpu.SemaphoreType.DMA(hung[:2]),
        ],
        compiler_params=pltpu.CompilerParams(
            vmem_limit_bytes=limit, collective_id=0, has_side_effects=True),
        cost_estimate=pl.CostEstimate(flops=16 * 10**9, bytes_accessed=16 << 20, transcendentals=0),
        name="channelize",
    )(*operands)
    kept = [kept[0].reshape(streams, 2, each, far, LANES), *kept[1:]]
    kept = [pltpu.with_memory_space_constraint(a, pltpu.VMEM) for a in kept]
    out = pl.pallas_call(
        functools.partial(deliver, parts),
        in_specs=[vmem] * 5,
        out_specs=hbm,
        out_shape=jax.ShapeDtypeStruct((streams, 2, each, rows * spans, LANES), jnp.float32),
        scratch_shapes=[
            pltpu.VMEM((2, each * (8 * spans + 8), LANES), jnp.float32),
            pltpu.SemaphoreType.DMA((streams, 2)),
            pltpu.SemaphoreType.DMA((2,)),
        ],
        compiler_params=pltpu.CompilerParams(vmem_limit_bytes=limit),
        cost_estimate=pl.CostEstimate(flops=10**7, bytes_accessed=16 << 20, transcendentals=0),
        name="deliver",
    )(*kept)
    out = out.reshape(streams, 2, tiles, spans, 8, LANES).transpose(0, 1, 2, 4, 3, 5)
    return out.reshape(streams, 2, 8 * tiles, spans * LANES)


def solution(mesh):
    in_specs = (P("stream", None, "tm"), P())
    out_specs = P("stream", None, "tm", None)
    body = functools.partial(shards, mesh.shape["tm"])
    return jax.shard_map(body, mesh=mesh, in_specs=in_specs, out_specs=out_specs, check_vma=False)
```

```python
import functools
import math

import jax
import jax.numpy as jnp
import numpy as np
from jax import lax
from jax.experimental import pallas as pl
from jax.experimental.pallas import tpu as pltpu
from jax.sharding import PartitionSpec as P

LANES = 128
GROUP = 4
BATCH = 2 * GROUP
SPAN = 32
CHUNK = 16
WIDE = 2 * LANES
POWER = 6
SCALE = 64.0


def angles(height, breadth, modulus):
    product = np.arange(height)[:, None] * np.arange(breadth)[None, :] % modulus
    return product * (2.0 * math.pi / modulus)


def split(table):
    high = table.astype(np.float32).astype(jnp.bfloat16)
    low = (table - high.astype(np.float64)).astype(np.float32).astype(jnp.bfloat16)
    return high, low


def first_table(rows):
    turn = angles(rows, rows, rows)
    cos, sin = np.cos(turn), np.sin(turn)
    whole = np.block([[cos, sin], [-sin, cos]])
    woven = whole.reshape(2 * rows, 2, rows).transpose(0, 2, 1).reshape(2 * rows, 2 * rows)
    high, low = split(np.kron(np.eye(GROUP), woven))
    return np.concatenate([high, low, high], axis=1)


def second_table(channels, parts):
    turn = angles(LANES, LANES, LANES)
    scale = 1.0 / math.isqrt(channels)
    cos, sin = np.cos(turn) * scale, np.sin(turn) * scale
    each = LANES // parts
    blocks = []
    for part in range(parts):
        pick = slice(part * each, (part + 1) * each)
        blocks.append(np.block([[cos[pick], sin[pick]], [-sin[pick], cos[pick]]]))
    high, low = split(np.concatenate(blocks, axis=0))
    table = np.concatenate([high, low, high], axis=1)
    return np.concatenate([table, table], axis=0)


def encode(value):
    value = value * SCALE
    square = value * jnp.abs(value)
    return (square * (square * square)).astype(jnp.bfloat16)


def decode(code):
    value = code.astype(jnp.float32)
    size = jnp.exp(jnp.log(jnp.abs(value)) * (1.0 / POWER)) * (1.0 / SCALE)
    return jnp.where(value < 0.0, -size, size)


def halves(value):
    high = value.astype(jnp.bfloat16)
    low = (value - high.astype(jnp.float32)).astype(jnp.bfloat16)
    return high, low


def equalize(parts, s, step, own, recv, own_over, recv_over, put):
    me = lax.axis_index("tm")
    blocks, each = own.shape[1], own.shape[5]
    fold = LANES // SPAN
    spans = blocks // fold
    quad = WIDE // SPAN
    group = own.shape[2] * quad // own_over.shape[1]
    over = WIDE // group
    lanes = lax.broadcasted_iota(jnp.int32, (CHUNK, LANES), 1)
    segment = lanes // SPAN
    ones = jnp.ones((2 * LANES, LANES), jnp.bfloat16)
    sources = [lax.rem(me + parts - k, parts) for k in range(parts)]

    def move(value, shift):
        return pltpu.roll(value, shift % LANES, 1) if shift % LANES else value

    for r in range(0, each, CHUNK):
        sub = slice(r, r + CHUNK)

        def fetch(k, b, j, p):
            if k == 0:
                return own[s, b, step, j, p, sub]
            return decode(recv[s, k - 1, b, step, j, p, sub])

        def hung(k, p):
            at, slot = step * quad // group, step * quad % group // (LANES // over)
            if k == 0:
                return own_over[s - 1, at, slot, p, sub]
            return decode(recv_over[s - 1, k - 1, at, slot, p, sub])

        if s > 0:
            extras = [[jnp.where(sources[k] > 0, hung((k + 1) % parts, p), 0.0)
                       for p in range(2)] for k in range(parts)]

        for j in range(WIDE // LANES):
            tiles = [[[fetch(k, b, j, p) for b in range(blocks)] for p in range(2)]
                     for k in range(parts)]
            merged, squares = [], []
            for i in range(fold):
                data = [[], []]
                for k in range(parts):
                    for p in range(2):
                        for u in range(spans):
                            value = tiles[k][p][u * fold]
                            for q in range(1, fold):
                                here = segment == (i + q) % fold
                                value = jnp.where(here, tiles[k][p][u * fold + q], value)
                            if s > 0 and u == 0:
                                extra = move(extras[k][p], -j * over)
                                inside = (segment == i) & (lanes % SPAN < over)
                                value = value + jnp.where(inside, extra, 0.0)
                            data[p].append(value)
                merged.append(data)
                squares.append(sum(a * a + b * b for a, b in zip(*data)))
            parted = jnp.concatenate(halves(jnp.concatenate(squares, axis=0)), axis=1)
            power = jnp.dot(parted, ones, preferred_element_type=jnp.float32)
            factor = lax.rsqrt(power * (1.0 / (parts * spans * LANES)) + 1.0)
            for i in range(fold):
                n = j * fold + i
                scale = factor[i * CHUNK : (i + 1) * CHUNK]
                for k in range(parts):
                    for p in range(2):
                        for u in range(spans):
                            value = merged[i][p][k * spans + u] * scale
                            put(p, step * quad + n, n, sources[k] * spans + u, r,
                                move(value, -i * SPAN))


def channelize(parts, streams, frames, rows, depth, x_hbm, taps_hbm, first_hbm, cos_hbm, sin_hbm,
               second_hbm, out_ref, own, recv, own_over, recv_over, xbuf, taps_raw, taps_ref,
               first_ref, cos_ref, sin_ref, second_ref, halo, wide, grid, zr, zi, send, send_over,
               x_sem, table_sem, halo_send, halo_recv, send_sem, recv_sem, over_send, over_recv):
    me = lax.axis_index("tm")
    each = LANES // parts
    past = depth - 1
    over = -(-past // BATCH) * BATCH
    blocks = frames // SPAN
    quad = WIDE // SPAN
    fold = LANES // SPAN
    steps = rows // quad
    group = WIDE // over
    spans = frames * parts // LANES
    reach = taps_ref.shape[0] // depth
    bounds = [max(b * SPAN - over, 0) for b in range(blocks)] + [frames]

    barrier = pltpu.get_barrier_semaphore()
    for k in range(1, parts):
        pl.semaphore_signal(barrier, inc=1, device_id={"tm": lax.rem(me + k, parts)},
                            device_id_type=pl.DeviceIdType.MESH)

    def load(s, b):
        pick = pl.ds(bounds[b], bounds[b + 1] - bounds[b])
        return pltpu.make_async_copy(x_hbm.at[s, pick], xbuf.at[pick], x_sem.at[b])

    def edge():
        return pltpu.make_async_remote_copy(
            src_ref=x_hbm.at[0, pl.ds(frames - past, past)], dst_ref=halo,
            send_sem=halo_send, recv_sem=halo_recv,
            device_id={"tm": lax.rem(me + 1, parts)}, device_id_type=pl.DeviceIdType.MESH)

    def piece(s, k, b, step):
        return pltpu.make_async_remote_copy(
            src_ref=send.at[s, k - 1, b, step], dst_ref=recv.at[s, k - 1, b, step],
            send_sem=send_sem.at[s, k - 1, b, step], recv_sem=recv_sem.at[s, k - 1, b, step],
            device_id={"tm": lax.rem(me + k, parts)}, device_id_type=pl.DeviceIdType.MESH)

    def overhang(s, k):
        return pltpu.make_async_remote_copy(
            src_ref=send_over.at[s - 1, k - 1], dst_ref=recv_over.at[s - 1, k - 1],
            send_sem=over_send.at[s - 1, k - 1], recv_sem=over_recv.at[s - 1, k - 1],
            device_id={"tm": lax.rem(me + k, parts)}, device_id_type=pl.DeviceIdType.MESH)

    load(0, blocks - 1).start()
    tables = [
        pltpu.make_async_copy(source, target, table_sem.at[i])
        for i, (source, target) in enumerate([
            (taps_hbm, taps_raw), (first_hbm, first_ref), (cos_hbm, cos_ref),
            (sin_hbm, sin_ref), (second_hbm, second_ref)])
    ]
    for table in tables:
        table.start()
    pl.semaphore_wait(barrier, parts - 1)

    @pl.when(me < parts - 1)
    def _():
        edge().start()

    for b in reversed(range(blocks - 1)):
        load(0, b).start()
    tables[0].wait()

    @pl.loop(0, rows)
    def _(n):
        for g in range(depth // 8):
            for p in range(2):
                row = pl.ds(g * 8 * reach + 2 * n + p, 8, stride=reach)
                taps_ref[row, :] = taps_raw[g, n]

    def widen(s, b):
        load(s, b).wait()

        @pl.loop(bounds[b] // BATCH, bounds[b + 1] // BATCH)
        def _(step):
            base = pl.multiple_of(step * BATCH, BATCH)
            wide[pl.ds(base + past, BATCH)] = xbuf[pl.ds(base, BATCH)].astype(jnp.float32)

    def first_stage(frame, slot, pitch):
        for block in range(2 * rows // 8):
            sub = slice(block * 8, block * 8 + 8)
            data = [wide[frame + i, sub, :] for i in range(BATCH + past)]
            taps = [taps_ref[k * reach + block * 8 : k * reach + block * 8 + 8, :]
                    for k in range(depth)]
            for t in range(BATCH):
                total = taps[0] * data[t + past]
                for k in range(1, depth):
                    total = total + taps[k] * data[t + past - k]
                row = (t % GROUP) * 2 * rows + block * 8
                lane = (t // GROUP) * LANES
                grid[row : row + 8, lane : lane + LANES] = total
        high, low = halves(grid[...])
        out = jnp.dot(first_ref[...], jnp.concatenate([high, high, low], axis=0),
                      preferred_element_type=jnp.float32)
        cos, sin = cos_ref[...], sin_ref[...]
        for t in range(BATCH):
            row = (t % GROUP) * 2 * rows
            lane = (t // GROUP) * LANES
            real = out[row : row + rows, lane : lane + LANES]
            imag = out[row + rows : row + 2 * rows, lane : lane + LANES]
            pick = pl.ds(slot + t, rows, stride=pitch)
            zr[pick, :] = real * cos + imag * sin
            zi[pick, :] = imag * cos - real * sin

    def second_stage(step, order, length, pitch):
        pieces = []
        for i in order:
            pick = pl.ds(pl.multiple_of((step * len(order) + i) * pitch, 8), length)
            pieces.append(jnp.concatenate([zr[pick, :], zi[pick, :]], axis=1))
        high, low = halves(jnp.concatenate(pieces, axis=0))
        top = pl.ds(pl.multiple_of(me * 2 * each, 2 * each), 2 * LANES)
        return lax.dot_general(second_ref[top, :], jnp.concatenate([high, high, low], axis=1),
                               (((1,), (1,)), ((), ())), preferred_element_type=jnp.float32)

    def keep(out, mine, theirs):
        for j in range(WIDE // LANES):
            lane = slice(j * LANES, (j + 1) * LANES)
            for p in range(2):
                mine[j, p] = out[p * each : (p + 1) * each, lane]
                for k in range(1, parts):
                    row = (2 * k + p) * each
                    theirs[k - 1][j, p] = encode(out[row : row + each, lane])

    def finish(s, step):
        for k in range(1, parts):
            for b in range(blocks):
                piece(s, k, b, step).wait_recv()
        pitch = out_ref.shape[2] // each

        def put(p, c, n, span, r, value):
            top = (c // 8) * (8 * spans) + span * 8 + n % 8
            out_ref[s, p, pl.ds(top + r * pitch, CHUNK, stride=pitch), :] = value

        equalize(parts, s, step, own, recv, own_over, recv_over, put)

    for s in range(streams):
        for b in reversed(range(blocks)):
            widen(s, b)
            if s > 0 and b == blocks - 2:

                @pl.when(me < parts - 1)
                def _():
                    for k in range(1, parts):
                        overhang(s, k).start()

            if b == 0:
                if s + 1 < streams:
                    for n in reversed(range(blocks)):
                        load(s + 1, n).start()
                if s == 0:

                    @pl.when(me > 0)
                    def _():
                        edge().wait_recv()
                        wide[:past] = halo[...].astype(jnp.float32)

                if s == 0:

                    @pl.when(me == 0)
                    def _():
                        wide[:past] = jnp.zeros((past, 2 * rows, LANES), jnp.float32)

                if s == 1:
                    wide[:past] = jnp.zeros((past, 2 * rows, LANES), jnp.float32)

            if s == 0 and b == blocks - 1:
                for table in tables[1:4]:
                    table.wait()

            @pl.loop(0, SPAN // BATCH)
            def _(step):
                base = pl.multiple_of(step * BATCH, BATCH)
                first_stage(b * SPAN + base, base, SPAN + 8)

            if s == 0 and b == blocks - 1:
                tables[4].wait()

            @pl.loop(0, steps)
            def _(step):
                order = [j + (i - b) % fold for j in range(0, quad, fold) for i in range(fold)]
                out = second_stage(step, order, SPAN, SPAN + 8)
                keep(out, own.at[s, b, step], [send.at[s, k, b, step] for k in range(parts - 1)])

                @pl.when(step > 0)
                def _():
                    for k in range(1, parts):
                        piece(s, k, b, step - 1).start()

            for k in range(1, parts):
                piece(s, k, b, steps - 1).start()

            if s == 1 and b == blocks - 1:
                wide[past + frames :] = jnp.zeros((over, 2 * rows, LANES), jnp.float32)

            if s > 0 and b == blocks - 1:

                @pl.loop(0, over // BATCH)
                def _(step):
                    base = pl.multiple_of(step * BATCH, BATCH)
                    first_stage(frames + base, base, over + 8)

                @pl.loop(0, rows // group)
                def _(step):
                    order = [j + i % 2 * fold + i // 2
                             for j in range(0, group, 2 * fold) for i in range(2 * fold)]
                    out = second_stage(step, order, over, over + 8)
                    keep(out, own_over.at[s - 1, step],
                         [send_over.at[s - 1, k, step] for k in range(parts - 1)])

    for s in range(streams):
        if s > 0:
            for k in range(1, parts):

                @pl.when(lax.rem(me + parts - k, parts) < parts - 1)
                def _():
                    overhang(s, k).wait_recv()

        early = steps if s + 1 < streams else steps - 8 // quad

        @pl.loop(0, early)
        def _(step):
            finish(s, step)

        @pl.loop(early, steps)
        def _(step):
            for k in range(1, parts):
                for b in range(blocks):
                    piece(s, k, b, step).wait_recv()

    for s in range(streams):

        @pl.loop(0, steps)
        def _(step):
            for k in range(1, parts):
                for b in range(blocks):
                    piece(s, k, b, step).wait_send()

    @pl.when(me < parts - 1)
    def _():
        edge().wait_send()
        for s in range(1, streams):
            for k in range(1, parts):
                overhang(s, k).wait_send()


def deliver(parts, planes, own, recv, own_over, recv_over, out_ref, tail, plane_sem, tail_sem):
    streams, each = own.shape[0], own.shape[5]
    rows = out_ref.shape[3]
    steps, quad = own.shape[2], WIDE // SPAN
    last = streams - 1
    spans = rows // (steps * quad)
    ready = rows - 8 * spans
    pitch = tail.shape[1] // each
    copies = []
    for s in range(streams):
        for p in range(2):
            pick = pl.ds(0, rows if s < last else ready)
            copies.append(pltpu.make_async_copy(
                planes.at[s, p, :, pick], out_ref.at[s, p, :, pick], plane_sem.at[s, p]))
    for copy in copies:
        copy.start()

    def put(p, c, n, span, r, value):
        tail[p, pl.ds(span * 8 + n % 8 + r * pitch, CHUNK, stride=pitch), :] = value

    @pl.loop(steps - 8 // quad, steps)
    def _(step):
        equalize(parts, last, step, own, recv, own_over, recv_over, put)

    for p in range(2):
        source = tail.at[p].reshape(each, pitch, LANES).at[:, pl.ds(0, 8 * spans)]
        copies.append(pltpu.make_async_copy(
            source, out_ref.at[last, p, :, pl.ds(ready, 8 * spans)], tail_sem.at[p]))
    for copy in copies[-2:]:
        copy.start()
    for copy in copies:
        copy.wait()


def shards(parts, signal, taps):
    streams = signal.shape[0]
    depth, channels = taps.shape
    rows = channels // LANES
    frames = signal.shape[2] // channels
    each = LANES // parts
    chunks = signal.shape[2] // LANES
    x = signal.reshape(streams, 2, chunks, LANES).transpose(0, 2, 1, 3)
    x = x.reshape(streams, frames, 2 * rows, LANES)
    taps = taps.reshape(depth // 8, 8, rows, LANES).transpose(0, 2, 1, 3)
    twist = angles(rows, LANES, channels)
    cos, sin = jnp.asarray(np.cos(twist), jnp.float32), jnp.asarray(np.sin(twist), jnp.float32)
    first = jnp.asarray(first_table(rows))
    second = jnp.asarray(second_table(channels, parts))
    blocks = frames // SPAN
    steps = rows * SPAN // WIDE
    over = -(-(depth - 1) // BATCH) * BATCH
    pitch = SPAN + 8
    reach = 2 * rows + 8
    spans = frames * parts // LANES
    tiles = channels // parts // 8
    width = 2 * rows * LANES * frames
    limit = (8 << 20) + 2 * width + 4 * width + 4 * width * 9 // 8 + 8 * width * streams * (parts + 1) // parts
    hbm = pl.BlockSpec(memory_space=pltpu.HBM)
    code = (streams, parts - 1, blocks, steps, WIDE // LANES, 2, each, LANES)
    hung = (streams - 1, parts - 1, rows * over // WIDE, WIDE // LANES, 2, each, LANES)
    operands = [x, taps, first, cos, sin, second]
    operands = [pltpu.with_memory_space_constraint(a, pltpu.HBM) for a in operands]
    far = rows * spans + 8
    vmem = pl.BlockSpec(memory_space=pltpu.VMEM)
    kept = pl.pallas_call(
        functools.partial(channelize, parts, streams, frames, rows, depth),
        in_specs=[hbm] * 6,
        out_specs=[vmem] * 5,
        out_shape=[
            pltpu.VMEM((streams, 2, each * far, LANES), jnp.float32),
            pltpu.VMEM(code[:1] + code[2:], jnp.float32),
            pltpu.VMEM(code, jnp.bfloat16),
            pltpu.VMEM(hung[:1] + hung[2:], jnp.float32),
            pltpu.VMEM(hung, jnp.bfloat16),
        ],
        scratch_shapes=[
            pltpu.VMEM((frames, 2 * rows, LANES), jnp.bfloat16),
            pltpu.VMEM(taps.shape, jnp.float32),
            pltpu.VMEM((depth * reach, LANES), jnp.float32),
            pltpu.VMEM(first.shape, jnp.bfloat16),
            pltpu.VMEM(cos.shape, jnp.float32),
            pltpu.VMEM(sin.shape, jnp.float32),
            pltpu.VMEM(second.shape, jnp.bfloat16),
            pltpu.VMEM((depth - 1, 2 * rows, LANES), jnp.bfloat16),
            pltpu.VMEM((depth - 1 + frames + over, 2 * rows, LANES), jnp.float32),
            pltpu.VMEM((2 * GROUP * rows, 2 * LANES), jnp.float32),
            pltpu.VMEM((rows * pitch, LANES), jnp.float32),
            pltpu.VMEM((rows * pitch, LANES), jnp.float32),
            pltpu.VMEM(code, jnp.bfloat16),
            pltpu.VMEM(hung, jnp.bfloat16),
            pltpu.SemaphoreType.DMA((blocks,)),
            pltpu.SemaphoreType.DMA((5,)),
            pltpu.SemaphoreType.DMA,
            pltpu.SemaphoreType.DMA,
            pltpu.SemaphoreType.DMA(code[:4]),
            pltpu.SemaphoreType.DMA(code[:4]),
            pltpu.SemaphoreType.DMA(hung[:2]),
            pltpu.SemaphoreType.DMA(hung[:2]),
        ],
        compiler_params=pltpu.CompilerParams(
            vmem_limit_bytes=limit, collective_id=0, has_side_effects=True),
        cost_estimate=pl.CostEstimate(flops=16 * 10**9, bytes_accessed=16 << 20, transcendentals=0),
        name="channelize",
    )(*operands)
    kept = [kept[0].reshape(streams, 2, each, far, LANES), *kept[1:]]
    kept = [pltpu.with_memory_space_constraint(a, pltpu.VMEM) for a in kept]
    out = pl.pallas_call(
        functools.partial(deliver, parts),
        in_specs=[vmem] * 5,
        out_specs=hbm,
        out_shape=jax.ShapeDtypeStruct((streams, 2, each, rows * spans, LANES), jnp.float32),
        scratch_shapes=[
            pltpu.VMEM((2, each * (8 * spans + 8), LANES), jnp.float32),
            pltpu.SemaphoreType.DMA((streams, 2)),
            pltpu.SemaphoreType.DMA((2,)),
        ],
        compiler_params=pltpu.CompilerParams(vmem_limit_bytes=limit),
        cost_estimate=pl.CostEstimate(flops=10**7, bytes_accessed=16 << 20, transcendentals=0),
        name="deliver",
    )(*kept)
    out = out.reshape(streams, 2, tiles, spans, 8, LANES).transpose(0, 1, 2, 4, 3, 5)
    return out.reshape(streams, 2, 8 * tiles, spans * LANES)


def solution(mesh):
    in_specs = (P("stream", None, "tm"), P())
    out_specs = P("stream", None, "tm", None)
    body = functools.partial(shards, mesh.shape["tm"])
    return jax.shard_map(body, mesh=mesh, in_specs=in_specs, out_specs=out_specs, check_vma=False)
```

```python
import functools
import math

import jax
import jax.numpy as jnp
import numpy as np
from jax import lax
from jax.experimental import pallas as pl
from jax.experimental.pallas import tpu as pltpu
from jax.sharding import PartitionSpec as P

LANES = 128
GROUP = 4
BATCH = 2 * GROUP
SPAN = 32
CHUNK = 16
WIDE = 2 * LANES
POWER = 6
SCALE = 64.0


def angles(height, breadth, modulus):
    product = np.arange(height)[:, None] * np.arange(breadth)[None, :] % modulus
    return product * (2.0 * math.pi / modulus)


def split(table):
    high = table.astype(np.float32).astype(jnp.bfloat16)
    low = (table - high.astype(np.float64)).astype(np.float32).astype(jnp.bfloat16)
    return high, low


def first_table(rows):
    turn = angles(rows, rows, rows)
    cos, sin = np.cos(turn), np.sin(turn)
    whole = np.block([[cos, sin], [-sin, cos]])
    woven = whole.reshape(2 * rows, 2, rows).transpose(0, 2, 1).reshape(2 * rows, 2 * rows)
    high, low = split(np.kron(np.eye(GROUP), woven))
    return np.concatenate([high, low, high], axis=1)


def second_table(channels, parts):
    turn = angles(LANES, LANES, LANES)
    scale = 1.0 / math.isqrt(channels)
    cos, sin = np.cos(turn) * scale, np.sin(turn) * scale
    each = LANES // parts
    blocks = []
    for part in range(parts):
        pick = slice(part * each, (part + 1) * each)
        blocks.append(np.block([[cos[pick], sin[pick]], [-sin[pick], cos[pick]]]))
    high, low = split(np.concatenate(blocks, axis=0))
    table = np.concatenate([high, low, high], axis=1)
    return np.concatenate([table, table], axis=0)


def encode(value):
    value = value * SCALE
    square = value * jnp.abs(value)
    return (square * (square * square)).astype(jnp.bfloat16)


def decode(code):
    value = code.astype(jnp.float32)
    size = jnp.exp(jnp.log(jnp.abs(value)) * (1.0 / POWER)) * (1.0 / SCALE)
    return jnp.where(value < 0.0, -size, size)


def halves(value):
    high = value.astype(jnp.bfloat16)
    low = (value - high.astype(jnp.float32)).astype(jnp.bfloat16)
    return high, low


def equalize(parts, s, step, own, recv, own_over, recv_over, put):
    me = lax.axis_index("tm")
    blocks, each = own.shape[1], own.shape[5]
    fold = LANES // SPAN
    spans = blocks // fold
    quad = WIDE // SPAN
    group = own.shape[2] * quad // own_over.shape[1]
    over = BATCH if s == 0 else WIDE // group
    lanes = lax.broadcasted_iota(jnp.int32, (CHUNK, LANES), 1)
    segment = lanes // SPAN
    ones = jnp.ones((2 * LANES, LANES), jnp.bfloat16)
    sources = [lax.rem(me + parts - k, parts) for k in range(parts)]

    def move(value, shift):
        return pltpu.roll(value, shift % LANES, 1) if shift % LANES else value

    for r in range(0, each, CHUNK):
        sub = slice(r, r + CHUNK)

        def fetch(k, b, j, p):
            if k == 0:
                return own[s, b, step, j, p, sub]
            return decode(recv[s, k - 1, b, step, j, p, sub])

        def hung(k, p):
            at, slot = (0, step // 2) if s == 0 else (step // 2, step % 2)
            if k == 0:
                return own_over[s, at, slot, p, sub]
            return decode(recv_over[s, k - 1, at, slot, p, sub])

        extras = [[jnp.where(sources[k] > 0, hung((k + 1) % parts, p), 0.0)
                   for p in range(2)] for k in range(parts)]

        for j in range(WIDE // LANES):
            tiles = [[[fetch(k, b, j, p) for b in range(blocks)] for p in range(2)]
                     for k in range(parts)]
            merged, squares = [], []
            for i in range(fold):
                data = [[], []]
                for k in range(parts):
                    for p in range(2):
                        for u in range(spans):
                            value = tiles[k][p][u * fold]
                            for q in range(1, fold):
                                here = segment == (i + q) % fold
                                value = jnp.where(here, tiles[k][p][u * fold + q], value)
                            if u == 0:
                                if s == 0:
                                    shift = LANES - (step % 2 * 2 + j) * over
                                    extra = pltpu.roll(extras[k][p], lax.rem(shift, LANES), 1)
                                else:
                                    extra = move(extras[k][p], -j * over)
                                inside = (segment == i) & (lanes % SPAN < over)
                                value = value + jnp.where(inside, extra, 0.0)
                            data[p].append(value)
                merged.append(data)
                squares.append(sum(a * a + b * b for a, b in zip(*data)))
            parted = jnp.concatenate(halves(jnp.concatenate(squares, axis=0)), axis=1)
            power = jnp.dot(parted, ones, preferred_element_type=jnp.float32)
            factor = lax.rsqrt(power * (1.0 / (parts * spans * LANES)) + 1.0)
            for i in range(fold):
                n = j * fold + i
                scale = factor[i * CHUNK : (i + 1) * CHUNK]
                for k in range(parts):
                    for p in range(2):
                        for u in range(spans):
                            value = merged[i][p][k * spans + u] * scale
                            put(p, step * quad + n, n, sources[k] * spans + u, r,
                                move(value, -i * SPAN))


def channelize(parts, streams, frames, rows, depth, x_hbm, taps_hbm, first_hbm, cos_hbm, sin_hbm,
               second_hbm, out_ref, own, recv, own_over, recv_over, xbuf, taps_raw, taps_ref,
               first_ref, cos_ref, sin_ref, second_ref, halo, wide, grid, zr, zi, send, send_over,
               x_sem, table_sem, halo_send, halo_recv, send_sem, recv_sem, over_send, over_recv):
    me = lax.axis_index("tm")
    each = LANES // parts
    past = depth - 1
    over = -(-past // BATCH) * BATCH
    near = past - BATCH
    blocks = frames // SPAN
    quad = WIDE // SPAN
    fold = LANES // SPAN
    steps = rows // quad
    spans = frames * parts // LANES
    reach = taps_ref.shape[0] // depth
    bounds = [max(b * SPAN - over, 0) for b in range(blocks)] + [frames]

    barrier = pltpu.get_barrier_semaphore()
    for k in range(1, parts):
        pl.semaphore_signal(barrier, inc=1, device_id={"tm": lax.rem(me + k, parts)},
                            device_id_type=pl.DeviceIdType.MESH)

    def load(s, b):
        pick = pl.ds(bounds[b], bounds[b + 1] - bounds[b])
        return pltpu.make_async_copy(x_hbm.at[s, pick], xbuf.at[pick], x_sem.at[b])

    def edge():
        return pltpu.make_async_remote_copy(
            src_ref=x_hbm.at[0, pl.ds(frames - near, near)], dst_ref=halo,
            send_sem=halo_send, recv_sem=halo_recv,
            device_id={"tm": lax.rem(me + 1, parts)}, device_id_type=pl.DeviceIdType.MESH)

    def piece(s, k, b, step):
        return pltpu.make_async_remote_copy(
            src_ref=send.at[s, k - 1, b, step], dst_ref=recv.at[s, k - 1, b, step],
            send_sem=send_sem.at[s, k - 1, b, step], recv_sem=recv_sem.at[s, k - 1, b, step],
            device_id={"tm": lax.rem(me + k, parts)}, device_id_type=pl.DeviceIdType.MESH)

    def overhang(s, k):
        units = rows * (BATCH if s == 0 else over) // WIDE
        return pltpu.make_async_remote_copy(
            src_ref=send_over.at[s, k - 1, pl.ds(0, units)],
            dst_ref=recv_over.at[s, k - 1, pl.ds(0, units)],
            send_sem=over_send.at[s, k - 1], recv_sem=over_recv.at[s, k - 1],
            device_id={"tm": lax.rem(me + k, parts)}, device_id_type=pl.DeviceIdType.MESH)

    load(0, blocks - 1).start()
    tables = [
        pltpu.make_async_copy(source, target, table_sem.at[i])
        for i, (source, target) in enumerate([
            (taps_hbm, taps_raw), (first_hbm, first_ref), (cos_hbm, cos_ref),
            (sin_hbm, sin_ref), (second_hbm, second_ref)])
    ]
    for table in tables:
        table.start()
    pl.semaphore_wait(barrier, parts - 1)

    @pl.when(me < parts - 1)
    def _():
        edge().start()

    for b in reversed(range(blocks - 1)):
        load(0, b).start()
    tables[0].wait()

    @pl.loop(0, rows)
    def _(n):
        for g in range(depth // 8):
            for p in range(2):
                row = pl.ds(g * 8 * reach + 2 * n + p, 8, stride=reach)
                taps_ref[row, :] = taps_raw[g, n]

    def widen(s, b):
        load(s, b).wait()

        @pl.loop(bounds[b] // BATCH, bounds[b + 1] // BATCH)
        def _(step):
            base = pl.multiple_of(step * BATCH, BATCH)
            wide[pl.ds(base + past, BATCH)] = xbuf[pl.ds(base, BATCH)].astype(jnp.float32)

    def first_stage(frame, slot, pitch):
        for block in range(2 * rows // 8):
            sub = slice(block * 8, block * 8 + 8)
            data = [wide[frame + i, sub, :] for i in range(BATCH + past)]
            taps = [taps_ref[k * reach + block * 8 : k * reach + block * 8 + 8, :]
                    for k in range(depth)]
            for t in range(BATCH):
                total = taps[0] * data[t + past]
                for k in range(1, depth):
                    total = total + taps[k] * data[t + past - k]
                row = (t % GROUP) * 2 * rows + block * 8
                lane = (t // GROUP) * LANES
                grid[row : row + 8, lane : lane + LANES] = total
        high, low = halves(grid[...])
        out = jnp.dot(first_ref[...], jnp.concatenate([high, high, low], axis=0),
                      preferred_element_type=jnp.float32)
        cos, sin = cos_ref[...], sin_ref[...]
        for t in range(BATCH):
            row = (t % GROUP) * 2 * rows
            lane = (t // GROUP) * LANES
            real = out[row : row + rows, lane : lane + LANES]
            imag = out[row + rows : row + 2 * rows, lane : lane + LANES]
            pick = pl.ds(slot + t, rows, stride=pitch)
            zr[pick, :] = real * cos + imag * sin
            zi[pick, :] = imag * cos - real * sin

    def second_stage(step, order, length, pitch):
        pieces = []
        for i in order:
            pick = pl.ds(pl.multiple_of((step * len(order) + i) * pitch, 8), length)
            pieces.append(jnp.concatenate([zr[pick, :], zi[pick, :]], axis=1))
        high, low = halves(jnp.concatenate(pieces, axis=0))
        top = pl.ds(pl.multiple_of(me * 2 * each, 2 * each), 2 * LANES)
        return lax.dot_general(second_ref[top, :], jnp.concatenate([high, high, low], axis=1),
                               (((1,), (1,)), ((), ())), preferred_element_type=jnp.float32)

    def keep(out, mine, theirs):
        for j in range(WIDE // LANES):
            lane = slice(j * LANES, (j + 1) * LANES)
            for p in range(2):
                mine[j, p] = out[p * each : (p + 1) * each, lane]
                for k in range(1, parts):
                    row = (2 * k + p) * each
                    theirs[k - 1][j, p] = encode(out[row : row + each, lane])

    def finish(s, step):
        for k in range(1, parts):
            for b in range(blocks):
                piece(s, k, b, step).wait_recv()
        pitch = out_ref.shape[2] // each

        def put(p, c, n, span, r, value):
            top = (c // 8) * (8 * spans) + span * 8 + n % 8
            out_ref[s, p, pl.ds(top + r * pitch, CHUNK, stride=pitch), :] = value

        equalize(parts, s, step, own, recv, own_over, recv_over, put)

    for s in range(streams):
        for b in reversed(range(blocks)):
            widen(s, b)
            if b == blocks - 2:

                @pl.when(me < parts - 1)
                def _():
                    for k in range(1, parts):
                        overhang(s, k).start()

            if b == 0:
                if s + 1 < streams:
                    for n in reversed(range(blocks)):
                        load(s + 1, n).start()
                if s == 0:

                    @pl.when(me > 0)
                    def _():
                        edge().wait_recv()
                        wide[BATCH:past] = halo[...].astype(jnp.float32)

                if s == 0:

                    @pl.when(me == 0)
                    def _():
                        wide[BATCH:past] = jnp.zeros((near, 2 * rows, LANES), jnp.float32)

                    wide[:BATCH] = jnp.zeros((BATCH, 2 * rows, LANES), jnp.float32)

                if s == 1:
                    wide[:past] = jnp.zeros((past, 2 * rows, LANES), jnp.float32)

            if s == 0 and b == blocks - 1:
                for table in tables[1:4]:
                    table.wait()

            @pl.loop(0, SPAN // BATCH)
            def _(step):
                base = pl.multiple_of(step * BATCH, BATCH)
                first_stage(b * SPAN + base, base, SPAN + 8)

            if s == 0 and b == blocks - 1:
                tables[4].wait()

            @pl.loop(0, steps)
            def _(step):
                order = [j + (i - b) % fold for j in range(0, quad, fold) for i in range(fold)]
                out = second_stage(step, order, SPAN, SPAN + 8)
                keep(out, own.at[s, b, step], [send.at[s, k, b, step] for k in range(parts - 1)])

                @pl.when(step > 0)
                def _():
                    for k in range(1, parts):
                        piece(s, k, b, step - 1).start()

            for k in range(1, parts):
                piece(s, k, b, steps - 1).start()

            if b == blocks - 1:
                if s == 0:
                    start, extent = past + frames, BATCH
                    old = pl.ds(frames - past, BATCH)
                    wide[start : start + BATCH] = xbuf[old].astype(jnp.float32)
                    wide[start + BATCH :] = jnp.zeros((past, 2 * rows, LANES), jnp.float32)
                    place = [(2 * t + m // 2) * quad + m % 2 * fold + i
                             for t in range(2) for i in range(fold) for m in range(fold)]
                else:
                    start, extent = frames, over
                    place = [j + i % 2 * fold + i // 2
                             for j in range(0, WIDE // over, 2 * fold) for i in range(2 * fold)]
                if s == 1:
                    wide[past + frames :] = jnp.zeros((past + BATCH, 2 * rows, LANES), jnp.float32)

                @pl.loop(0, extent // BATCH)
                def _(step):
                    base = pl.multiple_of(step * BATCH, BATCH)
                    first_stage(start + base, base, extent + 8)

                @pl.loop(0, rows * extent // WIDE)
                def _(step):
                    out = second_stage(step, place, extent, extent + 8)
                    keep(out, own_over.at[s, step],
                         [send_over.at[s, k, step] for k in range(parts - 1)])

    for s in range(streams):
        for k in range(1, parts):

            @pl.when(lax.rem(me + parts - k, parts) < parts - 1)
            def _():
                overhang(s, k).wait_recv()

        early = steps if s + 1 < streams else steps - 8 // quad

        @pl.loop(0, early)
        def _(step):
            finish(s, step)

        @pl.loop(early, steps)
        def _(step):
            for k in range(1, parts):
                for b in range(blocks):
                    piece(s, k, b, step).wait_recv()

    for s in range(streams):

        @pl.loop(0, steps)
        def _(step):
            for k in range(1, parts):
                for b in range(blocks):
                    piece(s, k, b, step).wait_send()

    @pl.when(me < parts - 1)
    def _():
        edge().wait_send()
        for s in range(streams):
            for k in range(1, parts):
                overhang(s, k).wait_send()


def deliver(parts, planes, own, recv, own_over, recv_over, out_ref, tail, plane_sem, tail_sem):
    streams, each = own.shape[0], own.shape[5]
    rows = out_ref.shape[3]
    steps, quad = own.shape[2], WIDE // SPAN
    last = streams - 1
    spans = rows // (steps * quad)
    ready = rows - 8 * spans
    pitch = tail.shape[1] // each
    copies = []
    for s in range(streams):
        for p in range(2):
            pick = pl.ds(0, rows if s < last else ready)
            copies.append(pltpu.make_async_copy(
                planes.at[s, p, :, pick], out_ref.at[s, p, :, pick], plane_sem.at[s, p]))
    for copy in copies:
        copy.start()

    def put(p, c, n, span, r, value):
        tail[p, pl.ds(span * 8 + n % 8 + r * pitch, CHUNK, stride=pitch), :] = value

    @pl.loop(steps - 8 // quad, steps)
    def _(step):
        equalize(parts, last, step, own, recv, own_over, recv_over, put)

    for p in range(2):
        source = tail.at[p].reshape(each, pitch, LANES).at[:, pl.ds(0, 8 * spans)]
        copies.append(pltpu.make_async_copy(
            source, out_ref.at[last, p, :, pl.ds(ready, 8 * spans)], tail_sem.at[p]))
    for copy in copies[-2:]:
        copy.start()
    for copy in copies:
        copy.wait()


def shards(parts, signal, taps):
    streams = signal.shape[0]
    depth, channels = taps.shape
    rows = channels // LANES
    frames = signal.shape[2] // channels
    each = LANES // parts
    chunks = signal.shape[2] // LANES
    x = signal.reshape(streams, 2, chunks, LANES).transpose(0, 2, 1, 3)
    x = x.reshape(streams, frames, 2 * rows, LANES)
    taps = taps.reshape(depth // 8, 8, rows, LANES).transpose(0, 2, 1, 3)
    twist = angles(rows, LANES, channels)
    cos, sin = jnp.asarray(np.cos(twist), jnp.float32), jnp.asarray(np.sin(twist), jnp.float32)
    first = jnp.asarray(first_table(rows))
    second = jnp.asarray(second_table(channels, parts))
    blocks = frames // SPAN
    steps = rows * SPAN // WIDE
    over = -(-(depth - 1) // BATCH) * BATCH
    pitch = SPAN + 8
    reach = 2 * rows + 8
    spans = frames * parts // LANES
    tiles = channels // parts // 8
    width = 2 * rows * LANES * frames
    limit = (8 << 20) + 2 * width + 4 * width + 4 * width * 9 // 8 + 8 * width * streams * (parts + 1) // parts
    hbm = pl.BlockSpec(memory_space=pltpu.HBM)
    code = (streams, parts - 1, blocks, steps, WIDE // LANES, 2, each, LANES)
    hung = (streams, parts - 1, rows * over // WIDE, WIDE // LANES, 2, each, LANES)
    operands = [x, taps, first, cos, sin, second]
    operands = [pltpu.with_memory_space_constraint(a, pltpu.HBM) for a in operands]
    far = rows * spans + 8
    vmem = pl.BlockSpec(memory_space=pltpu.VMEM)
    kept = pl.pallas_call(
        functools.partial(channelize, parts, streams, frames, rows, depth),
        in_specs=[hbm] * 6,
        out_specs=[vmem] * 5,
        out_shape=[
            pltpu.VMEM((streams, 2, each * far, LANES), jnp.float32),
            pltpu.VMEM(code[:1] + code[2:], jnp.float32),
            pltpu.VMEM(code, jnp.bfloat16),
            pltpu.VMEM(hung[:1] + hung[2:], jnp.float32),
            pltpu.VMEM(hung, jnp.bfloat16),
        ],
        scratch_shapes=[
            pltpu.VMEM((frames, 2 * rows, LANES), jnp.bfloat16),
            pltpu.VMEM(taps.shape, jnp.float32),
            pltpu.VMEM((depth * reach, LANES), jnp.float32),
            pltpu.VMEM(first.shape, jnp.bfloat16),
            pltpu.VMEM(cos.shape, jnp.float32),
            pltpu.VMEM(sin.shape, jnp.float32),
            pltpu.VMEM(second.shape, jnp.bfloat16),
            pltpu.VMEM((depth - 1 - BATCH, 2 * rows, LANES), jnp.bfloat16),
            pltpu.VMEM((2 * (depth - 1) + frames + BATCH, 2 * rows, LANES), jnp.float32),
            pltpu.VMEM((2 * GROUP * rows, 2 * LANES), jnp.float32),
            pltpu.VMEM((rows * pitch, LANES), jnp.float32),
            pltpu.VMEM((rows * pitch, LANES), jnp.float32),
            pltpu.VMEM(code, jnp.bfloat16),
            pltpu.VMEM(hung, jnp.bfloat16),
            pltpu.SemaphoreType.DMA((blocks,)),
            pltpu.SemaphoreType.DMA((5,)),
            pltpu.SemaphoreType.DMA,
            pltpu.SemaphoreType.DMA,
            pltpu.SemaphoreType.DMA(code[:4]),
            pltpu.SemaphoreType.DMA(code[:4]),
            pltpu.SemaphoreType.DMA(hung[:2]),
            pltpu.SemaphoreType.DMA(hung[:2]),
        ],
        compiler_params=pltpu.CompilerParams(
            vmem_limit_bytes=limit, collective_id=0, has_side_effects=True),
        cost_estimate=pl.CostEstimate(flops=16 * 10**9, bytes_accessed=16 << 20, transcendentals=0),
        name="channelize",
    )(*operands)
    kept = [kept[0].reshape(streams, 2, each, far, LANES), *kept[1:]]
    kept = [pltpu.with_memory_space_constraint(a, pltpu.VMEM) for a in kept]
    out = pl.pallas_call(
        functools.partial(deliver, parts),
        in_specs=[vmem] * 5,
        out_specs=hbm,
        out_shape=jax.ShapeDtypeStruct((streams, 2, each, rows * spans, LANES), jnp.float32),
        scratch_shapes=[
            pltpu.VMEM((2, each * (8 * spans + 8), LANES), jnp.float32),
            pltpu.SemaphoreType.DMA((streams, 2)),
            pltpu.SemaphoreType.DMA((2,)),
        ],
        compiler_params=pltpu.CompilerParams(vmem_limit_bytes=limit),
        cost_estimate=pl.CostEstimate(flops=10**7, bytes_accessed=16 << 20, transcendentals=0),
        name="deliver",
    )(*kept)
    out = out.reshape(streams, 2, tiles, spans, 8, LANES).transpose(0, 1, 2, 4, 3, 5)
    return out.reshape(streams, 2, 8 * tiles, spans * LANES)


def solution(mesh):
    in_specs = (P("stream", None, "tm"), P())
    out_specs = P("stream", None, "tm", None)
    body = functools.partial(shards, mesh.shape["tm"])
    return jax.shard_map(body, mesh=mesh, in_specs=in_specs, out_specs=out_specs, check_vma=False)
```

```python
import functools
import math

import jax
import jax.numpy as jnp
import numpy as np
from jax import lax
from jax.experimental import pallas as pl
from jax.experimental.pallas import tpu as pltpu
from jax.sharding import PartitionSpec as P

LANES = 128
GROUP = 4
BATCH = 2 * GROUP
SPAN = 32
CHUNK = 16
WIDE = 2 * LANES
POWER = 6
SCALE = 64.0


def angles(height, breadth, modulus):
    product = np.arange(height)[:, None] * np.arange(breadth)[None, :] % modulus
    return product * (2.0 * math.pi / modulus)


def split(table):
    high = table.astype(np.float32).astype(jnp.bfloat16)
    low = (table - high.astype(np.float64)).astype(np.float32).astype(jnp.bfloat16)
    return high, low


def first_table(rows):
    turn = angles(rows, rows, rows)
    cos, sin = np.cos(turn), np.sin(turn)
    whole = np.block([[cos, sin], [-sin, cos]])
    woven = whole.reshape(2 * rows, 2, rows).transpose(0, 2, 1).reshape(2 * rows, 2 * rows)
    high, low = split(np.kron(np.eye(GROUP), woven))
    return np.concatenate([high, low, high], axis=1)


def second_table(channels, parts):
    turn = angles(LANES, LANES, LANES)
    scale = 1.0 / math.isqrt(channels)
    cos, sin = np.cos(turn) * scale, np.sin(turn) * scale
    each = LANES // parts
    blocks = []
    for part in range(parts):
        pick = slice(part * each, (part + 1) * each)
        blocks.append(np.block([[cos[pick], sin[pick]], [-sin[pick], cos[pick]]]))
    high, low = split(np.concatenate(blocks, axis=0))
    table = np.concatenate([high, low, high], axis=1)
    return np.concatenate([table, table], axis=0)


def encode(value):
    value = value * SCALE
    square = value * jnp.abs(value)
    return (square * (square * square)).astype(jnp.bfloat16)


def decode(code):
    value = code.astype(jnp.float32)
    size = jnp.exp(jnp.log(jnp.abs(value)) * (1.0 / POWER)) * (1.0 / SCALE)
    return jnp.where(value < 0.0, -size, size)


def halves(value):
    high = value.astype(jnp.bfloat16)
    low = (value - high.astype(jnp.float32)).astype(jnp.bfloat16)
    return high, low


def equalize(parts, s, step, own, recv, own_over, recv_over, put):
    me = lax.axis_index("tm")
    blocks, each = own.shape[1], own.shape[5]
    fold = LANES // SPAN
    spans = blocks // fold
    quad = WIDE // SPAN
    group = own.shape[2] * quad // own_over.shape[1]
    over = BATCH if s == 0 else WIDE // group
    lanes = lax.broadcasted_iota(jnp.int32, (CHUNK, LANES), 1)
    segment = lanes // SPAN
    ones = jnp.ones((2 * LANES, LANES), jnp.bfloat16)
    sources = [lax.rem(me + parts - k, parts) for k in range(parts)]

    def move(value, shift):
        return pltpu.roll(value, shift % LANES, 1) if shift % LANES else value

    for r in range(0, each, CHUNK):
        sub = slice(r, r + CHUNK)

        def fetch(k, b, j, p):
            if k == 0:
                return own[s, b, step, j, p, sub]
            return decode(recv[s, k - 1, b, step, j, p, sub])

        def hung(k, p):
            at, slot = (0, step // 2) if s == 0 else (step // 2, step % 2)
            if k == 0:
                return own_over[s, at, slot, p, sub]
            return decode(recv_over[s, k - 1, at, slot, p, sub])

        extras = [[jnp.where(sources[k] > 0, hung((k + 1) % parts, p), 0.0)
                   for p in range(2)] for k in range(parts)]

        for j in range(WIDE // LANES):
            tiles = [[[fetch(k, b, j, p) for b in range(blocks)] for p in range(2)]
                     for k in range(parts)]
            merged, squares = [], []
            for i in range(fold):
                data = [[], []]
                for k in range(parts):
                    for p in range(2):
                        for u in range(spans):
                            value = tiles[k][p][u * fold]
                            for q in range(1, fold):
                                here = segment == (i + q) % fold
                                value = jnp.where(here, tiles[k][p][u * fold + q], value)
                            if u == 0:
                                if s == 0:
                                    shift = LANES - (step % 2 * 2 + j) * over
                                    extra = pltpu.roll(extras[k][p], lax.rem(shift, LANES), 1)
                                else:
                                    extra = move(extras[k][p], -j * over)
                                inside = (segment == i) & (lanes % SPAN < over)
                                value = value + jnp.where(inside, extra, 0.0)
                            data[p].append(value)
                merged.append(data)
                squares.append(sum(a * a + b * b for a, b in zip(*data)))
            parted = jnp.concatenate(halves(jnp.concatenate(squares, axis=0)), axis=1)
            power = jnp.dot(parted, ones, preferred_element_type=jnp.float32)
            factor = lax.rsqrt(power * (1.0 / (parts * spans * LANES)) + 1.0)
            for i in range(fold):
                n = j * fold + i
                scale = factor[i * CHUNK : (i + 1) * CHUNK]
                for k in range(parts):
                    for p in range(2):
                        for u in range(spans):
                            value = merged[i][p][k * spans + u] * scale
                            put(p, step * quad + n, n, sources[k] * spans + u, r,
                                move(value, -i * SPAN))


def channelize(parts, streams, frames, rows, depth, x_hbm, taps_hbm, first_hbm, cos_hbm, sin_hbm,
               second_hbm, out_ref, own, recv, own_over, recv_over, xbuf, taps_raw, taps_ref,
               first_ref, cos_ref, sin_ref, second_ref, halo, wide, grid, zr, zi, send, send_over,
               x_sem, table_sem, halo_send, halo_recv, send_sem, recv_sem, over_send, over_recv):
    me = lax.axis_index("tm")
    each = LANES // parts
    past = depth - 1
    over = -(-past // BATCH) * BATCH
    near = past - BATCH
    blocks = frames // SPAN
    quad = WIDE // SPAN
    fold = LANES // SPAN
    steps = rows // quad
    spans = frames * parts // LANES
    reach = taps_ref.shape[0] // depth
    bounds = [max(b * SPAN - over, 0) for b in range(blocks)] + [frames]

    barrier = pltpu.get_barrier_semaphore()
    for k in range(1, parts):
        pl.semaphore_signal(barrier, inc=1, device_id={"tm": lax.rem(me + k, parts)},
                            device_id_type=pl.DeviceIdType.MESH)

    def load(s, b):
        pick = pl.ds(bounds[b], bounds[b + 1] - bounds[b])
        return pltpu.make_async_copy(x_hbm.at[s, pick], xbuf.at[pick], x_sem.at[b])

    def edge():
        return pltpu.make_async_remote_copy(
            src_ref=x_hbm.at[0, pl.ds(frames - near, near)], dst_ref=halo,
            send_sem=halo_send, recv_sem=halo_recv,
            device_id={"tm": lax.rem(me + 1, parts)}, device_id_type=pl.DeviceIdType.MESH)

    def piece(s, k, b, step):
        return pltpu.make_async_remote_copy(
            src_ref=send.at[s, k - 1, b, step], dst_ref=recv.at[s, k - 1, b, step],
            send_sem=send_sem.at[s, k - 1, b, step], recv_sem=recv_sem.at[s, k - 1, b, step],
            device_id={"tm": lax.rem(me + k, parts)}, device_id_type=pl.DeviceIdType.MESH)

    def overhang(s, k):
        units = rows * (BATCH if s == 0 else over) // WIDE
        return pltpu.make_async_remote_copy(
            src_ref=send_over.at[s, k - 1, pl.ds(0, units)],
            dst_ref=recv_over.at[s, k - 1, pl.ds(0, units)],
            send_sem=over_send.at[s, k - 1], recv_sem=over_recv.at[s, k - 1],
            device_id={"tm": lax.rem(me + k, parts)}, device_id_type=pl.DeviceIdType.MESH)

    load(0, blocks - 1).start()
    tables = [
        pltpu.make_async_copy(source, target, table_sem.at[i])
        for i, (source, target) in enumerate([
            (taps_hbm, taps_raw), (first_hbm, first_ref), (cos_hbm, cos_ref),
            (sin_hbm, sin_ref), (second_hbm, second_ref)])
    ]
    for table in tables:
        table.start()
    for b in reversed(range(blocks - 1)):
        load(0, b).start()
    tables[0].wait()

    @pl.loop(0, rows, unroll=8)
    def _(n):
        for g in range(depth // 8):
            for p in range(2):
                row = pl.ds(g * 8 * reach + 2 * n + p, 8, stride=reach)
                taps_ref[row, :] = taps_raw[g, n]

    def widen(s, b):
        load(s, b).wait()

        @pl.loop(bounds[b] // BATCH, bounds[b + 1] // BATCH)
        def _(step):
            base = pl.multiple_of(step * BATCH, BATCH)
            wide[pl.ds(base + past, BATCH)] = xbuf[pl.ds(base, BATCH)].astype(jnp.float32)

    widen(0, blocks - 1)
    pl.semaphore_wait(barrier, parts - 1)

    @pl.when(me < parts - 1)
    def _():
        edge().start()

    def sift(frame, n):
        for block in range(2 * rows // 8):
            sub = slice(block * 8, block * 8 + 8)
            data = [wide[frame + i, sub, :] for i in range(BATCH + past)]
            taps = [taps_ref[k * reach + block * 8 : k * reach + block * 8 + 8, :]
                    for k in range(depth)]
            for t in range(BATCH):
                total = taps[0] * data[t + past]
                for k in range(1, depth):
                    total = total + taps[k] * data[t + past - k]
                row = (t % GROUP) * 2 * rows + block * 8
                lane = (t // GROUP) * LANES
                grid[n, row : row + 8, lane : lane + LANES] = total

    def turn(slot, pitch, n):
        high, low = halves(grid[n])
        out = jnp.dot(first_ref[...], jnp.concatenate([high, high, low], axis=0),
                      preferred_element_type=jnp.float32)
        cos, sin = cos_ref[...], sin_ref[...]
        for t in range(BATCH):
            row = (t % GROUP) * 2 * rows
            lane = (t // GROUP) * LANES
            real = out[row : row + rows, lane : lane + LANES]
            imag = out[row + rows : row + 2 * rows, lane : lane + LANES]
            pick = pl.ds(slot + t, rows, stride=pitch)
            zr[pick, :] = real * cos + imag * sin
            zi[pick, :] = imag * cos - real * sin

    def first_stage(frame, pitch, count):
        @pl.loop(0, count)
        def _(n):
            sift(frame + pl.multiple_of(n * BATCH, BATCH), n)

        @pl.loop(0, count, unroll=min(count, 4))
        def _(n):
            turn(pl.multiple_of(n * BATCH, BATCH), pitch, n)

    def second_stage(step, order, length, pitch):
        pieces = []
        for i in order:
            pick = pl.ds(pl.multiple_of((step * len(order) + i) * pitch, 8), length)
            pieces.append(jnp.concatenate([zr[pick, :], zi[pick, :]], axis=1))
        high, low = halves(jnp.concatenate(pieces, axis=0))
        top = pl.ds(pl.multiple_of(me * 2 * each, 2 * each), 2 * LANES)
        return lax.dot_general(second_ref[top, :], jnp.concatenate([high, high, low], axis=1),
                               (((1,), (1,)), ((), ())), preferred_element_type=jnp.float32)

    def keep(out, mine, theirs):
        for j in range(WIDE // LANES):
            lane = slice(j * LANES, (j + 1) * LANES)
            for p in range(2):
                mine[j, p] = out[p * each : (p + 1) * each, lane]
                for k in range(1, parts):
                    row = (2 * k + p) * each
                    theirs[k - 1][j, p] = encode(out[row : row + each, lane])

    def finish(s, step):
        for k in range(1, parts):
            for b in range(blocks):
                piece(s, k, b, step).wait_recv()
        pitch = out_ref.shape[2] // each

        def put(p, c, n, span, r, value):
            top = (c // 8) * (8 * spans) + span * 8 + n % 8
            out_ref[s, p, pl.ds(top + r * pitch, CHUNK, stride=pitch), :] = value

        equalize(parts, s, step, own, recv, own_over, recv_over, put)

    for s in range(streams):
        for b in reversed(range(blocks)):
            if s > 0 or b < blocks - 1:
                widen(s, b)
            if b == blocks - 2:

                @pl.when(me < parts - 1)
                def _():
                    for k in range(1, parts):
                        overhang(s, k).start()

            if b == 0:
                if s + 1 < streams:
                    for n in reversed(range(blocks)):
                        load(s + 1, n).start()
                if s == 0:

                    @pl.when(me > 0)
                    def _():
                        edge().wait_recv()
                        wide[BATCH:past] = halo[...].astype(jnp.float32)

                if s == 0:

                    @pl.when(me == 0)
                    def _():
                        wide[BATCH:past] = jnp.zeros((near, 2 * rows, LANES), jnp.float32)

                    wide[:BATCH] = jnp.zeros((BATCH, 2 * rows, LANES), jnp.float32)

                if s == 1:
                    wide[:past] = jnp.zeros((past, 2 * rows, LANES), jnp.float32)

            if s == 0 and b == blocks - 1:
                for table in tables[1:4]:
                    table.wait()

            first_stage(b * SPAN, SPAN + 8, SPAN // BATCH)

            if s == 0 and b == blocks - 1:
                tables[4].wait()

            @pl.loop(0, steps)
            def _(step):
                order = [j + (i - b) % fold for j in range(0, quad, fold) for i in range(fold)]
                out = second_stage(step, order, SPAN, SPAN + 8)
                keep(out, own.at[s, b, step], [send.at[s, k, b, step] for k in range(parts - 1)])

                @pl.when(step > 0)
                def _():
                    for k in range(1, parts):
                        piece(s, k, b, step - 1).start()

            for k in range(1, parts):
                piece(s, k, b, steps - 1).start()

            if b == blocks - 1:
                if s == 0:
                    start, extent = past + frames, BATCH
                    old = pl.ds(frames - past, BATCH)
                    wide[start : start + BATCH] = xbuf[old].astype(jnp.float32)
                    wide[start + BATCH :] = jnp.zeros((past, 2 * rows, LANES), jnp.float32)
                    place = [(2 * t + m // 2) * quad + m % 2 * fold + i
                             for t in range(2) for i in range(fold) for m in range(fold)]
                else:
                    start, extent = frames, over
                    place = [j + i % 2 * fold + i // 2
                             for j in range(0, WIDE // over, 2 * fold) for i in range(2 * fold)]
                if s == 1:
                    wide[past + frames :] = jnp.zeros((past + BATCH, 2 * rows, LANES), jnp.float32)

                first_stage(start, extent + 8, extent // BATCH)

                @pl.loop(0, rows * extent // WIDE)
                def _(step):
                    out = second_stage(step, place, extent, extent + 8)
                    keep(out, own_over.at[s, step],
                         [send_over.at[s, k, step] for k in range(parts - 1)])

    for s in range(streams):
        for k in range(1, parts):

            @pl.when(lax.rem(me + parts - k, parts) < parts - 1)
            def _():
                overhang(s, k).wait_recv()

        early = steps if s + 1 < streams else steps - 8 // quad

        @pl.loop(0, early)
        def _(step):
            finish(s, step)

        @pl.loop(early, steps)
        def _(step):
            for k in range(1, parts):
                for b in range(blocks):
                    piece(s, k, b, step).wait_recv()

    for s in range(streams):

        @pl.loop(0, steps)
        def _(step):
            for k in range(1, parts):
                for b in range(blocks):
                    piece(s, k, b, step).wait_send()

    @pl.when(me < parts - 1)
    def _():
        edge().wait_send()
        for s in range(streams):
            for k in range(1, parts):
                overhang(s, k).wait_send()


def deliver(parts, planes, own, recv, own_over, recv_over, out_ref, tail, plane_sem, tail_sem):
    streams, each = own.shape[0], own.shape[5]
    rows = out_ref.shape[3]
    steps, quad = own.shape[2], WIDE // SPAN
    last = streams - 1
    spans = rows // (steps * quad)
    ready = rows - 8 * spans
    pitch = tail.shape[1] // each
    copies = []
    for s in range(streams):
        for p in range(2):
            pick = pl.ds(0, rows if s < last else ready)
            copies.append(pltpu.make_async_copy(
                planes.at[s, p, :, pick], out_ref.at[s, p, :, pick], plane_sem.at[s, p]))
    for copy in copies:
        copy.start()

    def put(p, c, n, span, r, value):
        tail[p, pl.ds(span * 8 + n % 8 + r * pitch, CHUNK, stride=pitch), :] = value

    @pl.loop(steps - 8 // quad, steps)
    def _(step):
        equalize(parts, last, step, own, recv, own_over, recv_over, put)

    for p in range(2):
        source = tail.at[p].reshape(each, pitch, LANES).at[:, pl.ds(0, 8 * spans)]
        copies.append(pltpu.make_async_copy(
            source, out_ref.at[last, p, :, pl.ds(ready, 8 * spans)], tail_sem.at[p]))
    for copy in copies[-2:]:
        copy.start()
    for copy in copies:
        copy.wait()


def shards(parts, signal, taps):
    streams = signal.shape[0]
    depth, channels = taps.shape
    rows = channels // LANES
    frames = signal.shape[2] // channels
    each = LANES // parts
    chunks = signal.shape[2] // LANES
    x = signal.reshape(streams, 2, chunks, LANES).transpose(0, 2, 1, 3)
    x = x.reshape(streams, frames, 2 * rows, LANES)
    taps = taps.reshape(depth // 8, 8, rows, LANES).transpose(0, 2, 1, 3)
    twist = angles(rows, LANES, channels)
    cos, sin = jnp.asarray(np.cos(twist), jnp.float32), jnp.asarray(np.sin(twist), jnp.float32)
    first = jnp.asarray(first_table(rows))
    second = jnp.asarray(second_table(channels, parts))
    blocks = frames // SPAN
    steps = rows * SPAN // WIDE
    over = -(-(depth - 1) // BATCH) * BATCH
    pitch = SPAN + 8
    reach = 2 * rows + 8
    spans = frames * parts // LANES
    tiles = channels // parts // 8
    width = 2 * rows * LANES * frames
    limit = (8 << 20) + 2 * width + 4 * width + 4 * width * 9 // 8 + 8 * width * streams * (parts + 1) // parts
    hbm = pl.BlockSpec(memory_space=pltpu.HBM)
    code = (streams, parts - 1, blocks, steps, WIDE // LANES, 2, each, LANES)
    hung = (streams, parts - 1, rows * over // WIDE, WIDE // LANES, 2, each, LANES)
    operands = [x, taps, first, cos, sin, second]
    operands = [pltpu.with_memory_space_constraint(a, pltpu.HBM) for a in operands]
    far = rows * spans + 8
    vmem = pl.BlockSpec(memory_space=pltpu.VMEM)
    kept = pl.pallas_call(
        functools.partial(channelize, parts, streams, frames, rows, depth),
        in_specs=[hbm] * 6,
        out_specs=[vmem] * 5,
        out_shape=[
            pltpu.VMEM((streams, 2, each * far, LANES), jnp.float32),
            pltpu.VMEM(code[:1] + code[2:], jnp.float32),
            pltpu.VMEM(code, jnp.bfloat16),
            pltpu.VMEM(hung[:1] + hung[2:], jnp.float32),
            pltpu.VMEM(hung, jnp.bfloat16),
        ],
        scratch_shapes=[
            pltpu.VMEM((frames, 2 * rows, LANES), jnp.bfloat16),
            pltpu.VMEM(taps.shape, jnp.float32),
            pltpu.VMEM((depth * reach, LANES), jnp.float32),
            pltpu.VMEM(first.shape, jnp.bfloat16),
            pltpu.VMEM(cos.shape, jnp.float32),
            pltpu.VMEM(sin.shape, jnp.float32),
            pltpu.VMEM(second.shape, jnp.bfloat16),
            pltpu.VMEM((depth - 1 - BATCH, 2 * rows, LANES), jnp.bfloat16),
            pltpu.VMEM((2 * (depth - 1) + frames + BATCH, 2 * rows, LANES), jnp.float32),
            pltpu.VMEM((SPAN // BATCH, 2 * GROUP * rows, 2 * LANES), jnp.float32),
            pltpu.VMEM((rows * pitch, LANES), jnp.float32),
            pltpu.VMEM((rows * pitch, LANES), jnp.float32),
            pltpu.VMEM(code, jnp.bfloat16),
            pltpu.VMEM(hung, jnp.bfloat16),
            pltpu.SemaphoreType.DMA((blocks,)),
            pltpu.SemaphoreType.DMA((5,)),
            pltpu.SemaphoreType.DMA,
            pltpu.SemaphoreType.DMA,
            pltpu.SemaphoreType.DMA(code[:4]),
            pltpu.SemaphoreType.DMA(code[:4]),
            pltpu.SemaphoreType.DMA(hung[:2]),
            pltpu.SemaphoreType.DMA(hung[:2]),
        ],
        compiler_params=pltpu.CompilerParams(
            vmem_limit_bytes=limit, collective_id=0, has_side_effects=True),
        cost_estimate=pl.CostEstimate(flops=16 * 10**9, bytes_accessed=16 << 20, transcendentals=0),
        name="channelize",
    )(*operands)
    kept = [kept[0].reshape(streams, 2, each, far, LANES), *kept[1:]]
    kept = [pltpu.with_memory_space_constraint(a, pltpu.VMEM) for a in kept]
    out = pl.pallas_call(
        functools.partial(deliver, parts),
        in_specs=[vmem] * 5,
        out_specs=hbm,
        out_shape=jax.ShapeDtypeStruct((streams, 2, each, rows * spans, LANES), jnp.float32),
        scratch_shapes=[
            pltpu.VMEM((2, each * (8 * spans + 8), LANES), jnp.float32),
            pltpu.SemaphoreType.DMA((streams, 2)),
            pltpu.SemaphoreType.DMA((2,)),
        ],
        compiler_params=pltpu.CompilerParams(vmem_limit_bytes=limit),
        cost_estimate=pl.CostEstimate(flops=10**7, bytes_accessed=16 << 20, transcendentals=0),
        name="deliver",
    )(*kept)
    out = out.reshape(streams, 2, tiles, spans, 8, LANES).transpose(0, 1, 2, 4, 3, 5)
    return out.reshape(streams, 2, 8 * tiles, spans * LANES)


def solution(mesh):
    in_specs = (P("stream", None, "tm"), P())
    out_specs = P("stream", None, "tm", None)
    body = functools.partial(shards, mesh.shape["tm"])
    return jax.shard_map(body, mesh=mesh, in_specs=in_specs, out_specs=out_specs, check_vma=False)
```
